8 devices in a mesh: dp: 1 (over z), tp: 8 (over x, y, core).
Axes of the slice: x: 2, y: 2, z: 1, core: 2. Of those that a mesh axis runs over, the one named last changes fastest.
Arguments:
- x: bfloat16 [1792, 5120], P(('dp', 'tp'))
- dy: bfloat16 [1792, 5120], P(('dp', 'tp'))
- gate: bfloat16 [1792, 12288], P('dp', 'tp')
- up: bfloat16 [1792, 12288], P('dp', 'tp')
- w_gate: bfloat16 [5120, 12288], P(None, 'tp')
- w_up: bfloat16 [5120, 12288], P(None, 'tp')
- w_down: bfloat16 [12288, 5120], P('tp')
Outputs:
- output 1: bfloat16 [1792, 5120], P(('dp', 'tp'))
- output 2: bfloat16 [5120, 12288], P('dp', 'tp')
- output 3: bfloat16 [5120, 12288], P('dp', 'tp')
- output 4: bfloat16 [12288, 5120], P(('dp', 'tp'))
All inputs are finite; a program needn't handle non-finite values.
Results may differ from the reference program's by a relative error of at most 0.012.
Values are sent between devices in bfloat16 or wider.
A program may use at most 2 GiB of HBM per device.

```python
import jax
import jax.numpy as jnp

ROWS = 1792
D = 5120
FF = 12288


def act(gate, up):
    return jax.nn.silu(gate) * up


def setup_inputs(seed: int = 0, part: int = 0) -> dict:
    kx, ky, ka, kb, kg, ku, kd = jax.random.split(jax.random.key(seed), 7)
    kx, ky, ka, kb = (jax.random.fold_in(k, part) for k in (kx, ky, ka, kb))
    drawn = {
        "x": jax.random.normal(kx, (ROWS, D), jnp.float32),
        "dy": jax.random.normal(ky, (ROWS, D), jnp.float32),
        "gate": jax.random.normal(ka, (ROWS, FF), jnp.float32),
        "up": jax.random.normal(kb, (ROWS, FF), jnp.float32),
        "w_gate": jax.random.normal(kg, (D, FF), jnp.float32) * D**-0.5,
        "w_up": jax.random.normal(ku, (D, FF), jnp.float32) * D**-0.5,
        "w_down": jax.random.normal(kd, (FF, D), jnp.float32) * FF**-0.5,
    }
    return {k: v.astype(jnp.bfloat16) for k, v in drawn.items()}


def reference(x, dy, gate, up, w_gate, w_up, w_down):
    hidden, back = jax.vjp(act, gate.astype(jnp.float32), up.astype(jnp.float32))
    d_hidden = jnp.dot(dy, w_down.T, preferred_element_type=jnp.float32)
    d_gate, d_up = (g.astype(jnp.bfloat16) for g in back(d_hidden))
    dx = jnp.dot(d_gate, w_gate.T, preferred_element_type=jnp.float32) + jnp.dot(d_up, w_up.T, preferred_element_type=jnp.float32)
    dw_gate = jnp.dot(x.T, d_gate, preferred_element_type=jnp.float32)
    dw_up = jnp.dot(x.T, d_up, preferred_element_type=jnp.float32)
    dw_down = jnp.dot(hidden.astype(jnp.bfloat16).T, dy, preferred_element_type=jnp.float32)
    return tuple(g.astype(jnp.bfloat16) for g in (dx, dw_gate, dw_up, dw_down))
```

```python
import functools
import jax
import jax.numpy as jnp
from jax import lax
from jax.experimental import pallas as pl
from jax.experimental.pallas import tpu as pltpu

BF, F32 = jnp.bfloat16, jnp.float32
LIMIT = 62 * 1024 * 1024


def nt(a, b):
    return lax.dot_general(a, b, (((1,), (1,)), ((), ())), preferred_element_type=F32)


def tn(a, b):
    return lax.dot_general(a, b, (((0,), (0,)), ((), ())), preferred_element_type=F32)


def flipped(along_x, along_y, core):
    me = lax.axis_index("tp")
    return me + along_x * (4 - 8 * (me // 4)) + along_y * (2 - 4 * (me // 2 % 2)) + core * (1 - 2 * (me % 2))


def piece_row(g, k, half_rows):
    core = k // 2
    own = 2 * flipped(0, 0, core) + k % 2
    near = 2 * (flipped(1, 0, core) if k % 2 == 0 else flipped(0, 1, core))
    diag = 2 * flipped(1, 1, core) + k % 2
    return jnp.where(g == 0, own, jnp.where(g == 3, diag, near + g - 1))


def order(g, i, n):
    i = jnp.clip(i, 0, n - 1)
    return i + (g % 2) * (n - 1 - 2 * i)


def rows_kernel(n1, n2, tf, half, dy, *refs):
    gate, up = refs[:4], refs[4:8]
    wd, wg, wu, h_out, g_out, u_out, same, other, dyg, rows, dg, du, send, recv, local = refs[8:]
    g, i = pl.program_id(0), pl.program_id(1)
    last = n1 + n2 - 1
    n = 2 * half
    to_x, to_y, partner = ({"tp": flipped(*f)} for f in ((1, 0, 0), (0, 1, 0), (0, 0, 1)))

    def remote(k, src, dst, device):
        return pltpu.make_async_remote_copy(
            src_ref=src, dst_ref=dst, send_sem=send.at[k], recv_sem=recv.at[k], device_id=device, device_id_type=pl.DeviceIdType.MESH
        )

    lo, hi, first_n, last_n = pl.ds(0, half), pl.ds(half, half), pl.ds(0, n), pl.ds(n, n)
    own_swap = remote(0, dy, rows.at[0, last_n], partner)
    lo_x, lo_y = remote(1, dy.at[lo], rows.at[1, lo], to_x), remote(2, dy.at[lo], rows.at[1, hi], to_y)
    hi_x, hi_y = remote(3, dy.at[hi], rows.at[2, lo], to_x), remote(4, dy.at[hi], rows.at[2, hi], to_y)
    swap1, on_x = remote(5, rows.at[1, first_n], rows.at[1, last_n], partner), remote(6, rows.at[1, hi], rows.at[3, lo], to_x)
    swap2, on_y = remote(7, rows.at[2, first_n], rows.at[2, last_n], partner), remote(8, rows.at[2, lo], rows.at[3, hi], to_y)
    swap3 = remote(9, rows.at[3, first_n], rows.at[3, last_n], partner)
    take = pltpu.make_async_copy(dy, rows.at[0, first_n], local.at[4])
    keeps = [pltpu.make_async_copy(rows.at[k], dyg.at[pl.ds(2 * n * k, 2 * n)], local.at[k]) for k in range(4)]

    def at(group, step):
        return pl.when((g == group) & (i == step))

    @at(0, 0)
    def _():
        barrier = pltpu.get_barrier_semaphore()
        for device in (to_x, to_y, partner):
            pl.semaphore_signal(barrier, inc=1, device_id=device, device_id_type=pl.DeviceIdType.MESH)
        pl.semaphore_wait(barrier, 3)
        own_swap.start()
        take.start()
        lo_x.start()
        lo_y.start()
        take.wait()
        own_swap.wait_recv()
        keeps[0].start()

    @at(0, n1)
    def _():
        hi_x.start()
        hi_y.start()

    @at(0, last)
    def _():
        lo_x.wait_recv()
        lo_y.wait_recv()
        swap1.start()
        on_x.start()

    @at(1, 0)
    def _():
        swap1.wait_recv()
        keeps[1].start()

    @at(1, last)
    def _():
        hi_x.wait_recv()
        hi_y.wait_recv()
        swap2.start()
        on_y.start()

    @at(2, 0)
    def _():
        swap2.wait_recv()
        keeps[2].start()

    @at(2, last)
    def _():
        on_x.wait_recv()
        on_y.wait_recv()
        swap3.start()

    @at(3, 0)
    def _():
        swap3.wait_recv()
        keeps[3].start()

    @pl.when(i < n1)
    def _():
        dh = nt(rows[g], wd[...])
        here = pl.ds(pl.multiple_of(order(g, i, n1) * tf, tf), tf)
        for k in range(4):
            part = slice(k * half, (k + 1) * half)
            d = dh[part]
            a, u = gate[k][...].astype(F32), up[k][...].astype(F32)
            s = jax.nn.sigmoid(a)
            act = a * s
            h_out[part] = (act * u).astype(BF)
            dgate = (d * u * (s + act * (1 - s))).astype(BF)
            dup = (d * act).astype(BF)
            g_out[part] = dgate
            u_out[part] = dup
            dg[part, here] = dgate
            du[part, here] = dup

    @pl.when(i >= n1)
    def _():
        dx = nt(dg[...], wg[...]) + nt(du[...], wu[...])
        same[...] = dx[:n]
        other[...] = dx[n:].astype(BF)

    @at(3, last)
    def _():
        for copy in (own_swap, lo_x, lo_y, hi_x, hi_y, swap1, on_x, swap2, on_y, swap3):
            copy.wait_send()
        for copy in keeps:
            copy.wait()


def rows_call(dy, gate, up, w_down, w_gate, w_up, tf=256, td=512):
    n, d = dy.shape
    ff = w_down.shape[0]
    n1, n2, half = ff // tf, d // td, n // 2
    kept = [pl.BlockSpec((half, tf), functools.partial(lambda k, g, i: (piece_row(g, k, half), order(g, i, n1)), k)) for k in range(4)]
    ff_block = pl.BlockSpec((2 * n, tf), lambda g, i: (g, order(g, i, n1)))
    dx_block = pl.BlockSpec((n, td), lambda g, i: (g, order(g, i - n1, n2)))
    w_block = pl.BlockSpec((td, ff), lambda g, i: (order(g, i - n1, n2), 0))
    hbm = pl.BlockSpec(memory_space=pl.ANY)
    return pl.pallas_call(
        functools.partial(rows_kernel, n1, n2, tf, half),
        out_shape=[jax.ShapeDtypeStruct((8 * n, ff), BF)] * 3
        + [jax.ShapeDtypeStruct((4 * n, d), F32), jax.ShapeDtypeStruct((4 * n, d), BF), jax.ShapeDtypeStruct((8 * n, d), BF)],
        grid=(4, n1 + n2),
        in_specs=[hbm] + kept + kept + [pl.BlockSpec((tf, d), lambda g, i: (order(g, i, n1), 0)), w_block, w_block],
        out_specs=[ff_block] * 3 + [dx_block] * 2 + [hbm],
        scratch_shapes=[
            pltpu.VMEM((4, 2 * n, d), BF),
            pltpu.VMEM((2 * n, ff), BF),
            pltpu.VMEM((2 * n, ff), BF),
            pltpu.SemaphoreType.DMA((10,)),
            pltpu.SemaphoreType.DMA((10,)),
            pltpu.SemaphoreType.DMA((5,)),
        ],
        compiler_params=pltpu.CompilerParams(vmem_limit_bytes=LIMIT, collective_id=0, has_side_effects=True),
        cost_estimate=pl.CostEstimate(flops=48 * n * d * ff, bytes_accessed=24 * d * ff + 48 * n * (d + ff), transcendentals=8 * n * ff),
        name="rows",
    )(dy, *([gate] * 4), *([up] * 4), w_down, w_gate, w_up)


def weight_kernel(resident_left, nr, ns, tile, rpieces, spieces, *refs):
    res, stream = refs[:nr], refs[nr:nr + ns]
    out, kept, buf, rsem, ssem = refs[nr + ns:nr + ns + 5]
    left = refs[nr + ns + 5] if resident_left else None
    j, steps = pl.program_id(0), pl.num_programs(0)

    def res_copies():
        at = 0
        for k, (which, start, size) in enumerate(rpieces):
            yield pltpu.make_async_copy(res[which].at[pl.ds(start, size)], kept.at[pl.ds(at, size)], rsem.at[k])
            at += size

    def copies(step, slot):
        at = 0
        cols = pl.ds(pl.multiple_of(step * tile, tile), tile)
        for k, (which, start, size) in enumerate(spieces):
            yield pltpu.make_async_copy(stream[which].at[pl.ds(start, size), cols], buf.at[slot, pl.ds(at, size)], ssem.at[slot, k])
            at += size

    slot = lax.rem(j, 2)

    @pl.when(j == 0)
    def _():
        for c in res_copies():
            c.start()
        for c in copies(0, 0):
            c.start()

    @pl.when(j + 1 < steps)
    def _():
        for c in copies(j + 1, 1 - slot):
            c.start()

    @pl.when(j == 0)
    def _():
        for c in res_copies():
            c.wait()
        if resident_left:
            left[...] = kept[...].T

    for c in copies(j, slot):
        c.wait()
    if resident_left:
        out[...] = lax.dot_general(left[...], buf[slot], (((1,), (0,)), ((), ())), preferred_element_type=F32).astype(BF)
    else:
        out[...] = tn(buf[slot], kept[...]).astype(BF)


def weight_call(left, right, lpieces, rpieces, resident_left, tile=512):
    (res, kept_pieces), (stream, moved_pieces) = ((left, lpieces), (right, rpieces)) if resident_left else ((right, rpieces), (left, lpieces))
    rows, kept, wide = sum(p[2] for p in kept_pieces), res[0].shape[1], stream[0].shape[1]
    if resident_left:
        out_shape, out_spec = (kept, wide), pl.BlockSpec((kept, tile), lambda j: (0, j))
    else:
        out_shape, out_spec = (wide, kept), pl.BlockSpec((tile, kept), lambda j: (j, 0))
    scratch = [
        pltpu.VMEM((rows, kept), BF),
        pltpu.VMEM((2, rows, tile), BF),
        pltpu.SemaphoreType.DMA((len(kept_pieces),)),
        pltpu.SemaphoreType.DMA((2, len(moved_pieces))),
    ]
    if resident_left:
        scratch.append(pltpu.VMEM((kept, rows), BF))
    return pl.pallas_call(
        functools.partial(weight_kernel, resident_left, len(res), len(stream), tile, tuple(kept_pieces), tuple(moved_pieces)),
        out_shape=jax.ShapeDtypeStruct(out_shape, BF),
        grid=(wide // tile,),
        in_specs=[pl.BlockSpec(memory_space=pl.ANY)] * (len(res) + len(stream)),
        out_specs=out_spec,
        scratch_shapes=scratch,
        compiler_params=pltpu.CompilerParams(vmem_limit_bytes=LIMIT),
        cost_estimate=pl.CostEstimate(flops=2 * rows * kept * wide, bytes_accessed=2 * (rows * kept + rows * wide + kept * wide), transcendentals=0),
        name="weight",
    )(*res, *stream)


X, Y, CORE = 4, 2, 1


def solution(mesh):
    spec = jax.sharding.PartitionSpec
    rows, cols = spec(("dp", "tp"), None), spec("dp", "tp")

    def flip(a, bit):
        return lax.ppermute(a, "tp", [(k, k ^ bit) for k in range(8)])

    def step(x, dy, gate, up, w_gate, w_up, w_down):
        n = x.shape[0]
        half = n // 2
        hidden, d_gate, d_up, same, other, dys = rows_call(dy, gate, up, w_gate=w_gate, w_up=w_up, w_down=w_down)

        xx, xy = flip(x, X), flip(x, Y)
        xd1, xd2 = flip(xy[:half], X), flip(xx[half:], Y)
        xs = [x, xx, xy, xd1, xd2]
        xs += [flip(p, CORE) for p in xs]
        own, px, py, pd1, pd2 = 0, 1, 2, 3, 4
        pieces = [(own, 0, n), (own + 5, 0, n)]
        for at in (0, half):
            pieces += [(px, at, half), (py, at, half), (px + 5, at, half), (py + 5, at, half)]
        pieces += [(pd1, 0, half), (pd2, 0, half), (pd1 + 5, 0, half), (pd2 + 5, 0, half)]

        swapped = flip(other, CORE)

        def term(g, k, size=half):
            part = slice(g * n + k * half, g * n + k * half + size)
            return same[part] + swapped[part].astype(F32)

        r_lo, r_hi = flip(term(3, 0).astype(BF), X), flip(term(3, 1).astype(BF), Y)
        from_x, from_y = flip(term(1, 0).astype(BF), X), flip(term(2, 1).astype(BF), Y)
        last_lo = flip((term(1, 1) + r_lo.astype(F32)).astype(BF), Y)
        last_hi = flip((term(2, 0) + r_hi.astype(F32)).astype(BF), X)
        dx = term(0, 0, n) + jnp.concatenate([from_x, from_y]).astype(F32) + jnp.concatenate([last_lo, last_hi]).astype(F32)

        whole = [(0, 0, 8 * n)]
        dw_down = weight_call([hidden], [dys], whole, whole, True)
        dw_gate = weight_call(xs, [d_gate], pieces, whole, False)
        dw_up = weight_call(xs, [d_up], pieces, whole, False)
        return dx.astype(BF), dw_gate, dw_up, dw_down

    return jax.shard_map(
        step,
        mesh=mesh,
        in_specs=(rows, rows, cols, cols, spec(None, "tp"), spec(None, "tp"), spec("tp", None)),
        out_specs=(rows, cols, cols, rows),
        check_vma=False,
    )
```

```python
import functools
import jax
import jax.numpy as jnp
from jax import lax
from jax.experimental import pallas as pl
from jax.experimental.pallas import tpu as pltpu

BF, F32 = jnp.bfloat16, jnp.float32
LIMIT = 62 * 1024 * 1024


def nt(a, b):
    return lax.dot_general(a, b, (((1,), (1,)), ((), ())), preferred_element_type=F32)


def tn(a, b):
    return lax.dot_general(a, b, (((0,), (0,)), ((), ())), preferred_element_type=F32)


def flipped(along_x, along_y, core):
    me = lax.axis_index("tp")
    return me + along_x * (4 - 8 * (me // 4)) + along_y * (2 - 4 * (me // 2 % 2)) + core * (1 - 2 * (me % 2))


def piece_row(g, k):
    core = k // 2
    own = 2 * flipped(0, 0, core) + k % 2
    near = 2 * (flipped(1, 0, core) if k % 2 == 0 else flipped(0, 1, core))
    diag = 2 * flipped(1, 1, core) + k % 2
    return jnp.where(g == 0, own, jnp.where(g == 3, diag, near + g - 1))


def order(g, i, n):
    i = jnp.clip(i, 0, n - 1)
    return i + (g % 2) * (n - 1 - 2 * i)


def rows_kernel(n1, n2, tf, td, half, events, dy, x, gate, up, wd, wg, wu, *refs):
    h_out, g_out, u_out, same, swapped, dyg, xo, xa, xb, ya, yb = refs[:11]
    rows, gates, ups, hid, dg, du, stage, send, recv, local, gsem, osem = refs[11:]
    g, i = pl.program_id(0), pl.program_id(1)
    last = n1 + n2 - 1
    n = 2 * half
    to_x, to_y, partner = ({"tp": flipped(*f)} for f in ((1, 0, 0), (0, 1, 0), (0, 0, 1)))

    def remote(k, src, dst, device):
        return pltpu.make_async_remote_copy(
            src_ref=src, dst_ref=dst, send_sem=send.at[k], recv_sem=recv.at[k], device_id=device, device_id_type=pl.DeviceIdType.MESH
        )

    lo, hi, first_n, last_n = pl.ds(0, half), pl.ds(half, half), pl.ds(0, n), pl.ds(n, n)
    own_swap = remote(0, dy, rows.at[0, last_n], partner)
    lo_x, lo_y = remote(1, dy.at[lo], rows.at[1, lo], to_x), remote(2, dy.at[lo], rows.at[1, hi], to_y)
    hi_x, hi_y = remote(3, dy.at[hi], rows.at[2, lo], to_x), remote(4, dy.at[hi], rows.at[2, hi], to_y)
    swap1, on_x = remote(5, rows.at[1, first_n], rows.at[1, last_n], partner), remote(6, rows.at[1, hi], rows.at[3, lo], to_x)
    swap2, on_y = remote(7, rows.at[2, first_n], rows.at[2, last_n], partner), remote(8, rows.at[2, lo], rows.at[3, hi], to_y)
    swap3 = remote(9, rows.at[3, first_n], rows.at[3, last_n], partner)
    x_copies = [remote(10, x, xo, partner)]
    for src, at_x, at_y in ((x.at[lo], xa, ya), (x.at[hi], xb, yb)):
        k = 10 + len(x_copies)
        x_copies += [remote(k, src, at_x, to_x), remote(k + 1, src, at_y, to_y)]
    passes = []
    for group in range(4):
        final = 0 if group % 2 else (n2 - 1) * td
        early = pl.ds(td if group % 2 else 0, (n2 - 1) * td)
        out_rows = pl.ds(group * n, n)
        k = 15 + 2 * group
        passes.append([remote(k + j, stage.at[:, c], swapped.at[out_rows, c], partner) for j, c in enumerate((early, pl.ds(final, td)))])

    def kept(group):
        for k in range(4):
            at_rows = pl.ds(pl.multiple_of(piece_row(group, k) * half, half), half)
            for j, (ref, buf) in enumerate(((gate, gates), (up, ups))):
                yield pltpu.make_async_copy(ref.at[at_rows], buf.at[pl.ds(k * half, half)], gsem.at[j, k])

    def outs(group):
        for j, (buf, ref) in enumerate(((hid, h_out), (dg, g_out), (du, u_out))):
            yield pltpu.make_async_copy(buf, ref.at[pl.ds(pl.multiple_of(group * 2 * n, 2 * n), 2 * n)], osem.at[j])

    take = pltpu.make_async_copy(dy, rows.at[0, first_n], local.at[4])
    keeps = [pltpu.make_async_copy(rows.at[k], dyg.at[pl.ds(2 * n * k, 2 * n)], local.at[k]) for k in range(4)]

    def at(group, step):
        return pl.when((g == group) & (i == step))

    @at(0, 0)
    def _():
        barrier = pltpu.get_barrier_semaphore()
        for device in (to_x, to_y, partner):
            pl.semaphore_signal(barrier, inc=1, device_id=device, device_id_type=pl.DeviceIdType.MESH)
        pl.semaphore_wait(barrier, 3)
        own_swap.start()
        take.start()
        for copy in kept(0):
            copy.start()
        lo_x.start()
        lo_y.start()
        take.wait()
        own_swap.wait_recv()
        keeps[0].start()

    @at(0, events[0])
    def _():
        hi_x.start()
        hi_y.start()

    @at(0, events[1])
    def _():
        lo_x.wait_recv()
        lo_y.wait_recv()
        swap1.start()
        on_x.start()

    @at(1, 0)
    def _():
        swap1.wait_recv()
        keeps[1].start()

    @at(1, events[2])
    def _():
        hi_x.wait_recv()
        hi_y.wait_recv()
        swap2.start()
        on_y.start()
        for copy in x_copies:
            copy.start()

    @at(2, 0)
    def _():
        swap2.wait_recv()
        keeps[2].start()

    @at(2, events[3])
    def _():
        on_x.wait_recv()
        on_y.wait_recv()
        swap3.start()

    @at(3, 0)
    def _():
        swap3.wait_recv()
        keeps[3].start()

    for group in range(4):

        @at(group, last)
        def _(group=group):
            passes[group][0].start()

        @at(group + 1, 0)
        def _(group=group):
            passes[group][1].start()

        @at(group + 1, n1)
        def _(group=group):
            for copy in passes[group]:
                copy.wait_send()

    @pl.when(i == 0)
    def _():
        for copy in kept(g):
            copy.wait()

    @pl.when((i == 0) & (g > 0))
    def _():
        for copy in outs(g - 1):
            copy.wait()

    @pl.when(i == n1)
    def _():
        for copy in outs(g):
            copy.start()

    @pl.when((i == n1) & (g < 3))
    def _():
        for copy in kept(g + 1):
            copy.start()

    @pl.when(i < n1)
    def _():
        dh = nt(rows[g], wd[...])
        here = pl.ds(pl.multiple_of(order(g, i, n1) * tf, tf), tf)
        for k in range(4):
            part = slice(k * half, (k + 1) * half)
            d = dh[part]
            a, u = gates[part, here].astype(F32), ups[part, here].astype(F32)
            s = jax.nn.sigmoid(a)
            act = a * s
            hid[part, here] = (act * u).astype(BF)
            dg[part, here] = (d * u * (s + act * (1 - s))).astype(BF)
            du[part, here] = (d * act).astype(BF)

    @pl.when(i >= n1)
    def _():
        dx = nt(dg[...], wg[...]) + nt(du[...], wu[...])
        same[...] = dx[:n]
        stage[:, pl.ds(pl.multiple_of(order(g, i - n1, n2) * td, td), td)] = dx[n:].astype(BF)

    @at(3, last)
    def _():
        for copy in x_copies:
            copy.wait_recv()
        passes[3][1].start()
        for copy in (own_swap, lo_x, lo_y, hi_x, hi_y, swap1, on_x, swap2, on_y, swap3, *x_copies):
            copy.wait_send()
        for copy in keeps:
            copy.wait()
        for copy in outs(3):
            copy.wait()
        for copy in passes[3]:
            copy.wait_send()
        for pair in passes:
            for copy in pair:
                copy.wait_recv()


def rows_call(dy, x, gate, up, w_down, w_gate, w_up, tf=512, td=1024, events=(3, 7, 5, 5)):
    n, d = dy.shape
    ff = w_down.shape[0]
    n1, n2, half = ff // tf, d // td, n // 2
    dx_block = pl.BlockSpec((n, td), lambda g, i: (g, order(g, i - n1, n2)))
    w_block = pl.BlockSpec((td, ff), lambda g, i: (order(g, i - n1, n2), 0))
    hbm = pl.BlockSpec(memory_space=pl.ANY)
    return pl.pallas_call(
        functools.partial(rows_kernel, n1, n2, tf, td, half, events),
        out_shape=[jax.ShapeDtypeStruct((8 * n, ff), BF)] * 3
        + [jax.ShapeDtypeStruct((4 * n, d), F32), jax.ShapeDtypeStruct((4 * n, d), BF), jax.ShapeDtypeStruct((8 * n, d), BF), jax.ShapeDtypeStruct((n, d), BF)]
        + [jax.ShapeDtypeStruct((half, d), BF)] * 4,
        grid=(4, n1 + n2),
        in_specs=[hbm] * 4 + [pl.BlockSpec((tf, d), lambda g, i: (order(g, i, n1), 0)), w_block, w_block],
        out_specs=[hbm] * 3 + [dx_block] + [hbm] * 7,
        scratch_shapes=[
            pltpu.VMEM((4, 2 * n, d), BF),
            *[pltpu.VMEM((2 * n, ff), BF)] * 5,
            pltpu.VMEM((n, d), BF),
            pltpu.SemaphoreType.DMA((23,)),
            pltpu.SemaphoreType.DMA((23,)),
            pltpu.SemaphoreType.DMA((5,)),
            pltpu.SemaphoreType.DMA((2, 4)),
            pltpu.SemaphoreType.DMA((3,)),
        ],
        compiler_params=pltpu.CompilerParams(vmem_limit_bytes=LIMIT, collective_id=0, has_side_effects=True),
        cost_estimate=pl.CostEstimate(flops=48 * n * d * ff, bytes_accessed=24 * d * ff + 48 * n * (d + ff), transcendentals=8 * n * ff),
        name="rows",
    )(dy, x, gate, up, w_down, w_gate, w_up)


def weight_kernel(resident_left, nr, ns, tile, rpieces, spieces, sums, *refs):
    refs = list(refs)
    res, stream = [refs.pop(0) for _ in range(nr)], [refs.pop(0) for _ in range(ns)]
    addends = [[refs.pop(0) for _ in range(k)] for k in sums]
    out, *totals = [refs.pop(0) for _ in range(1 + len(sums))]
    kept, buf, rsem, ssem = refs[:4]
    left = refs[4] if resident_left else None
    j, steps = pl.program_id(0), pl.num_programs(0)

    def res_copies():
        at = 0
        for k, (which, start, size) in enumerate(rpieces):
            yield pltpu.make_async_copy(res[which].at[pl.ds(start, size)], kept.at[pl.ds(at, size)], rsem.at[k])
            at += size

    def copies(step, slot):
        at = 0
        cols = pl.ds(pl.multiple_of(step * tile, tile), tile)
        for k, (which, start, size) in enumerate(spieces):
            yield pltpu.make_async_copy(stream[which].at[pl.ds(start, size), cols], buf.at[slot, pl.ds(at, size)], ssem.at[slot, k])
            at += size

    slot = lax.rem(j, 2)

    @pl.when(j == 0)
    def _():
        for c in res_copies():
            c.start()
        for c in copies(0, 0):
            c.start()

    @pl.when(j + 1 < steps)
    def _():
        for c in copies(j + 1, 1 - slot):
            c.start()

    @pl.when(j == 0)
    def _():
        for c in res_copies():
            c.wait()
        if resident_left:
            left[...] = kept[...].T

    for c in copies(j, slot):
        c.wait()
    for total, parts in zip(totals, addends):
        total[...] = sum(p[...].astype(F32) for p in parts).astype(total.dtype)
    if resident_left:
        out[...] = lax.dot_general(left[...], buf[slot], (((1,), (0,)), ((), ())), preferred_element_type=F32).astype(BF)
    else:
        out[...] = tn(buf[slot], kept[...]).astype(BF)


def weight_call(left, right, lpieces, rpieces, resident_left, sums=(), tile=512):
    (res, kept_pieces), (stream, moved_pieces) = ((left, lpieces), (right, rpieces)) if resident_left else ((right, rpieces), (left, lpieces))
    rows, kept, wide = sum(p[2] for p in kept_pieces), res[0].shape[1], stream[0].shape[1]
    if resident_left:
        out_shape, out_spec = (kept, wide), pl.BlockSpec((kept, tile), lambda j: (0, j))
    else:
        out_shape, out_spec = (wide, kept), pl.BlockSpec((tile, kept), lambda j: (j, 0))
    scratch = [
        pltpu.VMEM((rows, kept), BF),
        pltpu.VMEM((2, rows, tile), BF),
        pltpu.SemaphoreType.DMA((len(kept_pieces),)),
        pltpu.SemaphoreType.DMA((2, len(moved_pieces))),
    ]
    if resident_left:
        scratch.append(pltpu.VMEM((kept, rows), BF))
    return pl.pallas_call(
        functools.partial(weight_kernel, resident_left, len(res), len(stream), tile, tuple(kept_pieces), tuple(moved_pieces), tuple(len(s[0]) for s in sums)),
        out_shape=[jax.ShapeDtypeStruct(out_shape, BF)] + [jax.ShapeDtypeStruct((size, wide), t) for _, size, t in sums],
        grid=(wide // tile,),
        in_specs=[pl.BlockSpec(memory_space=pl.ANY)] * (len(res) + len(stream))
        + [pl.BlockSpec((size, tile), functools.partial(lambda b, j: (b, j), b)) for parts, size, _ in sums for _, b in parts],
        out_specs=[out_spec] + [pl.BlockSpec((size, tile), lambda j: (0, j)) for _, size, _ in sums],
        scratch_shapes=scratch,
        compiler_params=pltpu.CompilerParams(vmem_limit_bytes=LIMIT),
        cost_estimate=pl.CostEstimate(flops=2 * rows * kept * wide, bytes_accessed=2 * (rows * kept + rows * wide + kept * wide), transcendentals=0),
        name="weight",
    )(*res, *stream, *[a for parts, _, _ in sums for a, _ in parts])


X, Y, CORE = 4, 2, 1


def solution(mesh):
    spec = jax.sharding.PartitionSpec
    rows, cols = spec(("dp", "tp"), None), spec("dp", "tp")

    def flip(a, bit):
        return lax.ppermute(a, "tp", [(k, k ^ bit) for k in range(8)])

    def step(x, dy, gate, up, w_gate, w_up, w_down):
        n = x.shape[0]
        half = n // 2
        tie = lax.optimization_barrier
        hidden, d_gate, d_up, same, swapped, dys, xo, xa, xb, ya, yb = rows_call(dy, x, gate, up, w_down, w_gate, w_up)

        fwd = [flip(ya, X), flip(xb, Y)]
        near = [flip(p, CORE) for p in (xa, ya, xb, yb)]
        def term(block, *more, dtype=BF):
            return ((same, block), (swapped, block), *((m, 0) for m in more)), half, dtype

        whole = [(0, 0, 8 * n)]
        dw_down, *diag, near_x, near_y = weight_call([hidden], [dys], whole, whole, True, [term(6), term(7), term(2), term(5)])
        *fwd, diag[0], diag[1] = tie((*fwd, *diag))
        r_lo, r_hi = flip(diag[0], X), flip(diag[1], Y)
        fwd += [flip(p, CORE) for p in fwd]
        *fwd, near_x, near_y = tie((*fwd, near_x, near_y))
        from_x, from_y = flip(near_x, X), flip(near_y, Y)
        xs = [x, xo, xa, ya, near[0], near[1], xb, yb, near[2], near[3], *fwd]
        pieces = [(k, 0, p.shape[0]) for k, p in enumerate(xs)]
        (dw_gate,) = weight_call(xs, [d_gate], pieces, whole, False)
        r_lo, r_hi, dw_gate = tie((r_lo, r_hi, dw_gate))

        def total(block, more):
            rows = slice(block * half, (block + 1) * half)
            return (same[rows] + swapped[rows].astype(F32) + more.astype(F32)).astype(BF)

        t_lo, t_hi, d_up = tie((total(3, r_lo), total(4, r_hi), d_up))
        last_lo, last_hi = flip(t_lo, Y), flip(t_hi, X)
        dw_up, base_lo, base_hi = weight_call(xs, [d_up], pieces, whole, False, [term(0, from_x, dtype=F32), term(1, from_y, dtype=F32)])
        dx = jnp.concatenate([base_lo + last_lo.astype(F32), base_hi + last_hi.astype(F32)])
        return dx.astype(BF), dw_gate, dw_up, dw_down

    return jax.shard_map(
        step,
        mesh=mesh,
        in_specs=(rows, rows, cols, cols, spec(None, "tp"), spec(None, "tp"), spec("tp", None)),
        out_specs=(rows, cols, cols, rows),
        check_vma=False,
    )
```

```python
import functools
import jax
import jax.numpy as jnp
from jax import lax
from jax.experimental import pallas as pl
from jax.experimental.pallas import tpu as pltpu

BF, F32 = jnp.bfloat16, jnp.float32
LIMIT = 62 * 1024 * 1024


def nt(a, b):
    return lax.dot_general(a, b, (((1,), (1,)), ((), ())), preferred_element_type=F32)


def tn(a, b):
    return lax.dot_general(a, b, (((0,), (0,)), ((), ())), preferred_element_type=F32)


def flipped(along_x, along_y, core):
    me = lax.axis_index("tp")
    return me + along_x * (4 - 8 * (me // 4)) + along_y * (2 - 4 * (me // 2 % 2)) + core * (1 - 2 * (me % 2))


def piece_row(g, k):
    core = k // 2
    own = 2 * flipped(0, 0, core) + k % 2
    near = 2 * (flipped(1, 0, core) if k % 2 == 0 else flipped(0, 1, core))
    diag = 2 * flipped(1, 1, core) + k % 2
    return jnp.where(g == 0, own, jnp.where(g == 3, diag, near + g - 1))


def order(g, i, n):
    i = jnp.clip(i, 0, n - 1)
    return i + (g % 2) * (n - 1 - 2 * i)


def rows_kernel(n1, n2, tf, td, half, events, dy, x, gate, up, wd, wg, wu, *refs):
    h_out, g_out, u_out, same, swapped, dyg, xo, xa, xb, ya, yb = refs[:11]
    rows, gates, ups, hid, dg, du, stage, send, recv, local, gsem, osem, wd_buf, w_buf, wd_sem, w_sem = refs[11:]
    g, i = pl.program_id(0), pl.program_id(1)
    last = n1 + n2 - 1
    n = 2 * half
    to_x, to_y, partner = ({"tp": flipped(*f)} for f in ((1, 0, 0), (0, 1, 0), (0, 0, 1)))

    def remote(k, src, dst, device):
        return pltpu.make_async_remote_copy(
            src_ref=src, dst_ref=dst, send_sem=send.at[k], recv_sem=recv.at[k], device_id=device, device_id_type=pl.DeviceIdType.MESH
        )

    lo, hi, first_n, last_n = pl.ds(0, half), pl.ds(half, half), pl.ds(0, n), pl.ds(n, n)
    own_swap = remote(0, dy, rows.at[0, last_n], partner)
    lo_x, lo_y = remote(1, dy.at[lo], rows.at[1, lo], to_x), remote(2, dy.at[lo], rows.at[1, hi], to_y)
    hi_x, hi_y = remote(3, dy.at[hi], rows.at[2, lo], to_x), remote(4, dy.at[hi], rows.at[2, hi], to_y)
    swap1, on_x = remote(5, rows.at[1, first_n], rows.at[1, last_n], partner), remote(6, rows.at[1, hi], rows.at[3, lo], to_x)
    swap2, on_y = remote(7, rows.at[2, first_n], rows.at[2, last_n], partner), remote(8, rows.at[2, lo], rows.at[3, hi], to_y)
    swap3 = remote(9, rows.at[3, first_n], rows.at[3, last_n], partner)
    x_copies = [remote(10, x, xo, partner)]
    for src, at_x, at_y in ((x.at[lo], xa, ya), (x.at[hi], xb, yb)):
        k = 10 + len(x_copies)
        x_copies += [remote(k, src, at_x, to_x), remote(k + 1, src, at_y, to_y)]
    passes = []
    for group in range(4):
        final = 0 if group % 2 else (n2 - 1) * td
        early = pl.ds(td if group % 2 else 0, (n2 - 1) * td)
        out_rows = pl.ds(group * n, n)
        k = 15 + 2 * group
        passes.append([remote(k + j, stage.at[:, c], swapped.at[out_rows, c], partner) for j, c in enumerate((early, pl.ds(final, td)))])

    def kept(group):
        for k in range(4):
            at_rows = pl.ds(pl.multiple_of(piece_row(group, k) * half, half), half)
            for j, (ref, buf) in enumerate(((gate, gates), (up, ups))):
                yield pltpu.make_async_copy(ref.at[at_rows], buf.at[pl.ds(k * half, half)], gsem.at[j, k])

    def outs(group):
        for j, (buf, ref) in enumerate(((hid, h_out), (dg, g_out), (du, u_out))):
            yield pltpu.make_async_copy(buf, ref.at[pl.ds(pl.multiple_of(group * 2 * n, 2 * n), 2 * n)], osem.at[j])

    def tiles(sources, buf, sem, count, size, q):
        turn, at = q // (count - 1), q % (count - 1)
        start = (at + turn % 2 * (count - 1 - 2 * at)) * size
        for k, ref in enumerate(sources):
            yield pltpu.make_async_copy(ref.at[pl.ds(pl.multiple_of(start, size), size)], buf.at[q % 2, k], sem.at[q % 2, k])

    q1, q2 = g * (n1 - 1) + i, g * (n2 - 1) + i - n1
    first_tiles, second_tiles = functools.partial(tiles, [wd], wd_buf, wd_sem, n1, tf), functools.partial(tiles, [wg, wu], w_buf, w_sem, n2, td)

    take = pltpu.make_async_copy(dy, rows.at[0, first_n], local.at[4])
    keeps = [pltpu.make_async_copy(rows.at[k], dyg.at[pl.ds(2 * n * k, 2 * n)], local.at[k]) for k in range(4)]

    def at(group, step):
        return pl.when((g == group) & (i == step))

    @at(0, 0)
    def _():
        barrier = pltpu.get_barrier_semaphore()
        for device in (to_x, to_y, partner):
            pl.semaphore_signal(barrier, inc=1, device_id=device, device_id_type=pl.DeviceIdType.MESH)
        pl.semaphore_wait(barrier, 3)
        own_swap.start()
        lo_x.start()
        lo_y.start()
        take.start()
        for copies in (first_tiles(0), kept(0), second_tiles(0)):
            for copy in copies:
                copy.start()
        take.wait()
        own_swap.wait_recv()
        keeps[0].start()

    @at(0, events[0])
    def _():
        hi_x.start()
        hi_y.start()

    @at(0, events[1])
    def _():
        lo_x.wait_recv()
        lo_y.wait_recv()
        swap1.start()
        on_x.start()

    @at(1, 0)
    def _():
        swap1.wait_recv()
        keeps[1].start()

    @at(1, events[2])
    def _():
        hi_x.wait_recv()
        hi_y.wait_recv()
        swap2.start()
        on_y.start()
        for copy in x_copies:
            copy.start()

    @at(2, 0)
    def _():
        swap2.wait_recv()
        keeps[2].start()

    @at(2, events[3])
    def _():
        on_x.wait_recv()
        on_y.wait_recv()
        swap3.start()

    @at(3, 0)
    def _():
        swap3.wait_recv()
        keeps[3].start()

    for group in range(4):

        @at(group, last)
        def _(group=group):
            passes[group][0].start()

        @at(group + 1, 0)
        def _(group=group):
            passes[group][1].start()

        @at(group + 1, n1)
        def _(group=group):
            for copy in passes[group]:
                copy.wait_send()

    @pl.when(i == 0)
    def _():
        for copy in kept(g):
            copy.wait()

    @pl.when((i == 0) & (g > 0))
    def _():
        for copy in outs(g - 1):
            copy.wait()

    @pl.when(i == n1)
    def _():
        for copy in outs(g):
            copy.start()

    @pl.when((i == n1) & (g < 3))
    def _():
        for copy in kept(g + 1):
            copy.start()

    @pl.when((i < n1) & ((g == 0) | (i > 0)))
    def _():
        for copy in first_tiles(q1):
            copy.wait()

        @pl.when(q1 < 4 * (n1 - 1))
        def _():
            for copy in first_tiles(q1 + 1):
                copy.start()

    @pl.when((i >= n1) & ((g == 0) | (i > n1)))
    def _():
        for copy in second_tiles(q2):
            copy.wait()

        @pl.when(q2 < 4 * (n2 - 1))
        def _():
            for copy in second_tiles(q2 + 1):
                copy.start()

    @pl.when(i < n1)
    def _():
        dh = nt(rows[g], wd_buf[q1 % 2, 0])
        here = pl.ds(pl.multiple_of(order(g, i, n1) * tf, tf), tf)
        for k in range(4):
            part = slice(k * half, (k + 1) * half)
            d = dh[part]
            a, u = gates[part, here].astype(F32), ups[part, here].astype(F32)
            s = jax.nn.sigmoid(a)
            act = a * s
            hid[part, here] = (act * u).astype(BF)
            dg[part, here] = (d * u * (s + act * (1 - s))).astype(BF)
            du[part, here] = (d * act).astype(BF)

    @pl.when(i >= n1)
    def _():
        dx = nt(dg[...], w_buf[q2 % 2, 0]) + nt(du[...], w_buf[q2 % 2, 1])
        same[...] = dx[:n]
        stage[:, pl.ds(pl.multiple_of(order(g, i - n1, n2) * td, td), td)] = dx[n:].astype(BF)

    @at(3, last)
    def _():
        for copy in x_copies:
            copy.wait_recv()
        passes[3][1].start()
        for copy in (own_swap, lo_x, lo_y, hi_x, hi_y, swap1, on_x, swap2, on_y, swap3, *x_copies):
            copy.wait_send()
        for copy in keeps:
            copy.wait()
        for copy in outs(3):
            copy.wait()
        for copy in passes[3]:
            copy.wait_send()
        for pair in passes:
            for copy in pair:
                copy.wait_recv()


def rows_call(dy, x, gate, up, w_down, w_gate, w_up, tf=512, td=1024, events=(3, 7, 5, 5)):
    n, d = dy.shape
    ff = w_down.shape[0]
    n1, n2, half = ff // tf, d // td, n // 2
    dx_block = pl.BlockSpec((n, td), lambda g, i: (g, order(g, i - n1, n2)))
    hbm = pl.BlockSpec(memory_space=pl.ANY)
    return pl.pallas_call(
        functools.partial(rows_kernel, n1, n2, tf, td, half, events),
        out_shape=[jax.ShapeDtypeStruct((8 * n, ff), BF)] * 3
        + [jax.ShapeDtypeStruct((4 * n, d), F32), jax.ShapeDtypeStruct((4 * n, d), BF), jax.ShapeDtypeStruct((8 * n, d), BF), jax.ShapeDtypeStruct((n, d), BF)]
        + [jax.ShapeDtypeStruct((half, d), BF)] * 4,
        grid=(4, n1 + n2),
        in_specs=[hbm] * 7,
        out_specs=[hbm] * 3 + [dx_block] + [hbm] * 7,
        scratch_shapes=[
            pltpu.VMEM((4, 2 * n, d), BF),
            *[pltpu.VMEM((2 * n, ff), BF)] * 5,
            pltpu.VMEM((n, d), BF),
            pltpu.SemaphoreType.DMA((23,)),
            pltpu.SemaphoreType.DMA((23,)),
            pltpu.SemaphoreType.DMA((5,)),
            pltpu.SemaphoreType.DMA((2, 4)),
            pltpu.SemaphoreType.DMA((3,)),
            pltpu.VMEM((2, 1, tf, d), BF),
            pltpu.VMEM((2, 2, td, ff), BF),
            pltpu.SemaphoreType.DMA((2, 1)),
            pltpu.SemaphoreType.DMA((2, 2)),
        ],
        compiler_params=pltpu.CompilerParams(vmem_limit_bytes=LIMIT, collective_id=0, has_side_effects=True),
        cost_estimate=pl.CostEstimate(flops=48 * n * d * ff, bytes_accessed=24 * d * ff + 48 * n * (d + ff), transcendentals=8 * n * ff),
        name="rows",
    )(dy, x, gate, up, w_down, w_gate, w_up)


def weight_kernel(resident_left, nr, ns, tile, rpieces, spieces, sums, *refs):
    refs = list(refs)
    res, stream = [refs.pop(0) for _ in range(nr)], [refs.pop(0) for _ in range(ns)]
    addends = [[refs.pop(0) for _ in range(k)] for k in sums]
    out, *totals = [refs.pop(0) for _ in range(1 + len(sums))]
    kept, buf, rsem, ssem = refs[:4]
    left = refs[4] if resident_left else None
    j, steps = pl.program_id(0), pl.num_programs(0)

    chunk = kept.shape[1] // 3

    def res_copies(m):
        at, part = 0, pl.ds(m * chunk, chunk)
        for k, (which, start, size) in enumerate(rpieces):
            yield pltpu.make_async_copy(res[which].at[pl.ds(start, size), part], kept.at[pl.ds(at, size), part], rsem.at[k, m])
            at += size

    def copies(step, slot):
        at = 0
        cols = pl.ds(pl.multiple_of(step * tile, tile), tile)
        for k, (which, start, size) in enumerate(spieces):
            yield pltpu.make_async_copy(stream[which].at[pl.ds(start, size), cols], buf.at[slot, pl.ds(at, size)], ssem.at[slot, k])
            at += size

    slot = lax.rem(j, 2)

    @pl.when(j == 0)
    def _():
        for c in copies(0, 0):
            c.start()
        for m in range(3):
            for c in res_copies(m):
                c.start()

    @pl.when(j + 1 < steps)
    def _():
        for c in copies(j + 1, 1 - slot):
            c.start()

    for c in copies(j, slot):
        c.wait()
    for total, parts in zip(totals, addends):
        total[...] = sum(p[...].astype(F32) for p in parts).astype(total.dtype)

    if not resident_left:

        @pl.when(j == 0)
        def _():
            for m in range(3):
                for c in res_copies(m):
                    c.wait()

        out[...] = tn(buf[slot], kept[...]).astype(BF)
        return

    @pl.when(j == 0)
    def _():
        for m in range(3):
            for c in res_copies(m):
                c.wait()
            part = slice(m * chunk, (m + 1) * chunk)
            left[part] = kept[:, part].T
            out[part] = jnp.dot(left[part], buf[slot], preferred_element_type=F32).astype(BF)

    @pl.when(j > 0)
    def _():
        out[...] = jnp.dot(left[...], buf[slot], preferred_element_type=F32).astype(BF)


def weight_call(left, right, lpieces, rpieces, resident_left, sums=(), tile=512):
    (res, kept_pieces), (stream, moved_pieces) = ((left, lpieces), (right, rpieces)) if resident_left else ((right, rpieces), (left, lpieces))
    rows, kept, wide = sum(p[2] for p in kept_pieces), res[0].shape[1], stream[0].shape[1]
    if resident_left:
        out_shape, out_spec = (kept, wide), pl.BlockSpec((kept, tile), lambda j: (0, j))
    else:
        out_shape, out_spec = (wide, kept), pl.BlockSpec((tile, kept), lambda j: (j, 0))
    scratch = [
        pltpu.VMEM((rows, kept), BF),
        pltpu.VMEM((2, rows, tile), BF),
        pltpu.SemaphoreType.DMA((len(kept_pieces), 3)),
        pltpu.SemaphoreType.DMA((2, len(moved_pieces))),
    ]
    if resident_left:
        scratch.append(pltpu.VMEM((kept, rows), BF))
    return pl.pallas_call(
        functools.partial(weight_kernel, resident_left, len(res), len(stream), tile, tuple(kept_pieces), tuple(moved_pieces), tuple(len(s[0]) for s in sums)),
        out_shape=[jax.ShapeDtypeStruct(out_shape, BF)] + [jax.ShapeDtypeStruct((size, wide), t) for _, size, t in sums],
        grid=(wide // tile,),
        in_specs=[pl.BlockSpec(memory_space=pl.ANY)] * (len(res) + len(stream))
        + [pl.BlockSpec((size, tile), functools.partial(lambda b, j: (b, j), b)) for parts, size, _ in sums for _, b in parts],
        out_specs=[out_spec] + [pl.BlockSpec((size, tile), lambda j: (0, j)) for _, size, _ in sums],
        scratch_shapes=scratch,
        compiler_params=pltpu.CompilerParams(vmem_limit_bytes=LIMIT),
        cost_estimate=pl.CostEstimate(flops=2 * rows * kept * wide, bytes_accessed=2 * (rows * kept + rows * wide + kept * wide), transcendentals=0),
        name="weight",
    )(*res, *stream, *[a for parts, _, _ in sums for a, _ in parts])


def finish_kernel(base, *refs):
    *parts, out = refs
    half = out.shape[0] // 2
    for k in range(2):
        rows = slice(k * half, (k + 1) * half)
        out[rows] = (base[rows] + parts[2 * k][...].astype(F32) + parts[2 * k + 1][...].astype(F32)).astype(BF)


def finish_call(base, first, second, tile=1024):
    n, d = base.shape
    piece = pl.BlockSpec((n // 2, tile), lambda j: (0, j))
    row = pl.BlockSpec((n, tile), lambda j: (0, j))
    return pl.pallas_call(
        finish_kernel,
        out_shape=jax.ShapeDtypeStruct((n, d), BF),
        grid=(d // tile,),
        in_specs=[row] + [piece] * 4,
        out_specs=row,
        cost_estimate=pl.CostEstimate(flops=2 * n * d, bytes_accessed=10 * n * d, transcendentals=0),
        name="finish",
    )(base, *first, *second)


X, Y, CORE = 4, 2, 1


def solution(mesh):
    spec = jax.sharding.PartitionSpec
    rows, cols = spec(("dp", "tp"), None), spec("dp", "tp")

    def flip(a, bit):
        return lax.ppermute(a, "tp", [(k, k ^ bit) for k in range(8)])

    def step(x, dy, gate, up, w_gate, w_up, w_down):
        n = x.shape[0]
        half = n // 2
        tie = lax.optimization_barrier
        hidden, d_gate, d_up, same, swapped, dys, xo, xa, xb, ya, yb = rows_call(dy, x, gate, up, w_down, w_gate, w_up)

        fwd = [flip(ya, X), flip(xb, Y)]
        near = [flip(p, CORE) for p in (xa, ya, xb, yb)]
        def term(block):
            return ((same, block), (swapped, block)), half, BF

        whole = [(0, 0, 8 * n)]
        dw_down, *diag, near_x, near_y = weight_call([hidden], [dys], whole, whole, True, [term(6), term(7), term(2), term(5)])
        *fwd, near[0], near[1], near[2], near[3], diag[0], diag[1] = tie((*fwd, *near, *diag))
        r_lo, r_hi = flip(diag[0], X), flip(diag[1], Y)
        fwd += [flip(p, CORE) for p in fwd]
        *fwd, near_x, near_y = tie((*fwd, near_x, near_y))
        from_x, from_y = flip(near_x, X), flip(near_y, Y)
        xs = [x, xo, xa, ya, near[0], near[1], xb, yb, near[2], near[3], *fwd]
        pieces = [(k, 0, p.shape[0]) for k, p in enumerate(xs)]
        (dw_gate,) = weight_call(xs, [d_gate], pieces, whole, False)
        r_lo, r_hi, dw_gate = tie((r_lo, r_hi, dw_gate))

        def total(block, more):
            rows = slice(block * half, (block + 1) * half)
            return (same[rows] + swapped[rows].astype(F32) + more.astype(F32)).astype(BF)

        t_lo, t_hi, d_up = tie((total(3, r_lo), total(4, r_hi), d_up))
        last_lo, last_hi = flip(t_lo, Y), flip(t_hi, X)
        dw_up, base = weight_call(xs, [d_up], pieces, whole, False, [(((same, 0), (swapped, 0)), n, F32)])
        return finish_call(base, (from_x, last_lo), (from_y, last_hi)), dw_gate, dw_up, dw_down

    return jax.shard_map(
        step,
        mesh=mesh,
        in_specs=(rows, rows, cols, cols, spec(None, "tp"), spec(None, "tp"), spec("tp", None)),
        out_specs=(rows, cols, cols, rows),
        check_vma=False,
    )
```

```python
import functools
import jax
import jax.numpy as jnp
from jax import lax
from jax.experimental import pallas as pl
from jax.experimental.pallas import tpu as pltpu

BF, F32 = jnp.bfloat16, jnp.float32
LIMIT = 62 * 1024 * 1024


def nt(a, b):
    return lax.dot_general(a, b, (((1,), (1,)), ((), ())), preferred_element_type=F32)


def tn(a, b):
    return lax.dot_general(a, b, (((0,), (0,)), ((), ())), preferred_element_type=F32)


def flipped(along_x, along_y, core):
    me = lax.axis_index("tp")
    return me + along_x * (4 - 8 * (me // 4)) + along_y * (2 - 4 * (me // 2 % 2)) + core * (1 - 2 * (me % 2))


def piece_row(g, k):
    core = k // 2
    own = 2 * flipped(0, 0, core) + k % 2
    near = 2 * (flipped(1, 0, core) if k % 2 == 0 else flipped(0, 1, core))
    diag = 2 * flipped(1, 1, core) + k % 2
    return jnp.where(g == 0, own, jnp.where(g == 3, diag, near + g - 1))


def order(g, i, n):
    i = jnp.clip(i, 0, n - 1)
    return i + (g % 2) * (n - 1 - 2 * i)


def rows_kernel(n1, n2, tf, td, half, events, dy, x, gate, up, wd, wg, wu, *refs):
    h_out, g_out, u_out, same, swapped, dyg, xo, xa, xb, ya, yb = refs[:11]
    rows, gates, ups, hid, dg, du, stage, send, recv, local, gsem, osem, acc, wd_buf, w_buf, wd_sem, w_sem = refs[11:]
    g, i = pl.program_id(0), pl.program_id(1)
    last = n1 + n2 - 1
    n = 2 * half
    to_x, to_y, partner = ({"tp": flipped(*f)} for f in ((1, 0, 0), (0, 1, 0), (0, 0, 1)))

    def remote(k, src, dst, device):
        return pltpu.make_async_remote_copy(
            src_ref=src, dst_ref=dst, send_sem=send.at[k], recv_sem=recv.at[k], device_id=device, device_id_type=pl.DeviceIdType.MESH
        )

    lo, hi, first_n, last_n = pl.ds(0, half), pl.ds(half, half), pl.ds(0, n), pl.ds(n, n)
    own_swap = remote(0, dy, rows.at[0, last_n], partner)
    lo_x, lo_y = remote(1, dy.at[lo], rows.at[1, lo], to_x), remote(2, dy.at[lo], rows.at[1, hi], to_y)
    hi_x, hi_y = remote(3, dy.at[hi], rows.at[2, lo], to_x), remote(4, dy.at[hi], rows.at[2, hi], to_y)
    swap1, on_x = remote(5, rows.at[1, first_n], rows.at[1, last_n], partner), remote(6, rows.at[1, hi], rows.at[3, lo], to_x)
    swap2, on_y = remote(7, rows.at[2, first_n], rows.at[2, last_n], partner), remote(8, rows.at[2, lo], rows.at[3, hi], to_y)
    swap3 = remote(9, rows.at[3, first_n], rows.at[3, last_n], partner)
    x_copies = [remote(10, x, xo, partner)]
    for src, at_x, at_y in ((x.at[lo], xa, ya), (x.at[hi], xb, yb)):
        k = 10 + len(x_copies)
        x_copies += [remote(k, src, at_x, to_x), remote(k + 1, src, at_y, to_y)]
    passes = []
    for group in range(4):
        final = 0 if group % 2 else (n2 - 1) * td
        early = pl.ds(td if group % 2 else 0, (n2 - 1) * td)
        out_rows = pl.ds(group * n, n)
        k = 15 + 2 * group
        passes.append([remote(k + j, stage.at[:, c], swapped.at[out_rows, c], partner) for j, c in enumerate((early, pl.ds(final, td)))])

    def kept(group):
        for k in range(4):
            at_rows = pl.ds(pl.multiple_of(piece_row(group, k) * half, half), half)
            for j, (ref, buf) in enumerate(((gate, gates), (up, ups))):
                yield pltpu.make_async_copy(ref.at[at_rows], buf.at[pl.ds(k * half, half)], gsem.at[j, k])

    def outs(group):
        for j, (buf, ref) in enumerate(((hid, h_out), (dg, g_out), (du, u_out))):
            yield pltpu.make_async_copy(buf, ref.at[pl.ds(pl.multiple_of(group * 2 * n, 2 * n), 2 * n)], osem.at[j])

    def tiles(sources, buf, sem, count, size, q):
        turn, at = q // (count - 1), q % (count - 1)
        start = (at + turn % 2 * (count - 1 - 2 * at)) * size
        for k, ref in enumerate(sources):
            yield pltpu.make_async_copy(ref.at[pl.ds(pl.multiple_of(start, size), size)], buf.at[q % 2, k], sem.at[q % 2, k])

    q1, q2 = g * (n1 - 1) + i, g * (n2 - 1) + i - n1
    first_tiles, second_tiles = functools.partial(tiles, [wd], wd_buf, wd_sem, n1, tf), functools.partial(tiles, [wg, wu], w_buf, w_sem, n2, td)

    take = pltpu.make_async_copy(dy, rows.at[0, first_n], local.at[4])
    keeps = [pltpu.make_async_copy(rows.at[k], dyg.at[pl.ds(2 * n * k, 2 * n)], local.at[k]) for k in range(4)]

    def at(group, step):
        return pl.when((g == group) & (i == step))

    @at(0, 0)
    def _():
        barrier = pltpu.get_barrier_semaphore()
        for device in (to_x, to_y, partner):
            pl.semaphore_signal(barrier, inc=1, device_id=device, device_id_type=pl.DeviceIdType.MESH)
        pl.semaphore_wait(barrier, 3)
        own_swap.start()
        lo_x.start()
        lo_y.start()
        take.start()
        for copies in (first_tiles(0), kept(0), second_tiles(0)):
            for copy in copies:
                copy.start()
        take.wait()
        own_swap.wait_recv()
        keeps[0].start()

    @at(0, events[0])
    def _():
        hi_x.start()
        hi_y.start()

    @at(0, events[1])
    def _():
        lo_x.wait_recv()
        lo_y.wait_recv()
        swap1.start()
        on_x.start()

    @at(1, 0)
    def _():
        swap1.wait_recv()
        keeps[1].start()

    @at(1, events[2])
    def _():
        hi_x.wait_recv()
        hi_y.wait_recv()
        swap2.start()
        on_y.start()
        for copy in x_copies:
            copy.start()

    @at(2, 0)
    def _():
        swap2.wait_recv()
        keeps[2].start()

    @at(2, events[3])
    def _():
        on_x.wait_recv()
        on_y.wait_recv()
        swap3.start()

    @at(3, 0)
    def _():
        swap3.wait_recv()
        keeps[3].start()

    for group in range(4):

        @at(group, last)
        def _(group=group):
            passes[group][0].start()

        @at(group + 1, 0)
        def _(group=group):
            passes[group][1].start()

        @at(group + 1, n1)
        def _(group=group):
            for copy in passes[group]:
                copy.wait_send()

    @pl.when(i == 0)
    def _():
        for copy in kept(g):
            copy.wait()

    @pl.when((i == 0) & (g > 0))
    def _():
        for copy in outs(g - 1):
            copy.wait()

    @pl.when(i == n1 + 1)
    def _():
        for copy in outs(g):
            copy.start()

    @pl.when((i == n1 + 1) & (g < 3))
    def _():
        for copy in kept(g + 1):
            copy.start()

    def activate(step):
        here = pl.ds(pl.multiple_of(order(g, step, n1) * tf, tf), tf)
        for k in range(4):
            part = slice(k * half, (k + 1) * half)
            d = acc[(step + 2) % 2, part]
            a, u = gates[part, here].astype(F32), ups[part, here].astype(F32)
            s = jax.nn.sigmoid(a)
            act = a * s
            hid[part, here] = (act * u).astype(BF)
            dg[part, here] = (d * u * (s + act * (1 - s))).astype(BF)
            du[part, here] = (d * act).astype(BF)

    @pl.when((i < n1) & ((g == 0) | (i > 0)))
    def _():
        for copy in first_tiles(q1):
            copy.wait()

        @pl.when(q1 < 4 * (n1 - 1))
        def _():
            for copy in first_tiles(q1 + 1):
                copy.start()

    @pl.when((i >= n1) & ((g == 0) | (i > n1)))
    def _():
        for copy in second_tiles(q2):
            copy.wait()

        @pl.when(q2 < 4 * (n2 - 1))
        def _():
            for copy in second_tiles(q2 + 1):
                copy.start()

    @pl.when(i < n1)
    def _():
        acc[i % 2] = nt(rows[g], wd_buf[q1 % 2, 0])
        activate(i - 1)

    @pl.when(i == n1)
    def _():
        activate(n1 - 1)

    @pl.when(i >= n1)
    def _():
        dx = nt(dg[...], w_buf[q2 % 2, 0]) + nt(du[...], w_buf[q2 % 2, 1])
        same[...] = dx[:n]
        stage[:, pl.ds(pl.multiple_of(order(g, i - n1, n2) * td, td), td)] = dx[n:].astype(BF)

    @at(3, last)
    def _():
        for copy in x_copies:
            copy.wait_recv()
        passes[3][1].start()
        for copy in (own_swap, lo_x, lo_y, hi_x, hi_y, swap1, on_x, swap2, on_y, swap3, *x_copies):
            copy.wait_send()
        for copy in keeps:
            copy.wait()
        for copy in outs(3):
            copy.wait()
        for copy in passes[3]:
            copy.wait_send()
        for pair in passes:
            for copy in pair:
                copy.wait_recv()


def rows_call(dy, x, gate, up, w_down, w_gate, w_up, tf=512, td=1024, events=(3, 7, 5, 5)):
    n, d = dy.shape
    ff = w_down.shape[0]
    n1, n2, half = ff // tf, d // td, n // 2
    dx_block = pl.BlockSpec((n, td), lambda g, i: (g, order(g, i - n1, n2)))
    hbm = pl.BlockSpec(memory_space=pl.ANY)
    return pl.pallas_call(
        functools.partial(rows_kernel, n1, n2, tf, td, half, events),
        out_shape=[jax.ShapeDtypeStruct((8 * n, ff), BF)] * 3
        + [jax.ShapeDtypeStruct((4 * n, d), F32), jax.ShapeDtypeStruct((4 * n, d), BF), jax.ShapeDtypeStruct((8 * n, d), BF), jax.ShapeDtypeStruct((n, d), BF)]
        + [jax.ShapeDtypeStruct((half, d), BF)] * 4,
        grid=(4, n1 + n2),
        in_specs=[hbm] * 7,
        out_specs=[hbm] * 3 + [dx_block] + [hbm] * 7,
        scratch_shapes=[
            pltpu.VMEM((4, 2 * n, d), BF),
            *[pltpu.VMEM((2 * n, ff), BF)] * 5,
            pltpu.VMEM((n, d), BF),
            pltpu.SemaphoreType.DMA((23,)),
            pltpu.SemaphoreType.DMA((23,)),
            pltpu.SemaphoreType.DMA((5,)),
            pltpu.SemaphoreType.DMA((2, 4)),
            pltpu.SemaphoreType.DMA((3,)),
            pltpu.VMEM((2, 2 * n, tf), F32),
            pltpu.VMEM((2, 1, tf, d), BF),
            pltpu.VMEM((2, 2, td, ff), BF),
            pltpu.SemaphoreType.DMA((2, 1)),
            pltpu.SemaphoreType.DMA((2, 2)),
        ],
        compiler_params=pltpu.CompilerParams(vmem_limit_bytes=LIMIT, collective_id=0, has_side_effects=True),
        cost_estimate=pl.CostEstimate(flops=48 * n * d * ff, bytes_accessed=24 * d * ff + 48 * n * (d + ff), transcendentals=8 * n * ff),
        name="rows",
    )(dy, x, gate, up, w_down, w_gate, w_up)


def weight_kernel(resident_left, nr, ns, tile, rpieces, spieces, sums, *refs):
    refs = list(refs)
    res, stream = [refs.pop(0) for _ in range(nr)], [refs.pop(0) for _ in range(ns)]
    addends = [[refs.pop(0) for _ in range(k)] for k in sums]
    out, *totals = [refs.pop(0) for _ in range(1 + len(sums))]
    kept, buf, rsem, ssem, left = refs
    j, steps = pl.program_id(0), pl.num_programs(0)

    chunk = kept.shape[1] // 3

    def res_copies(m):
        at, part = 0, pl.ds(m * chunk, chunk)
        for k, (which, start, size) in enumerate(rpieces):
            yield pltpu.make_async_copy(res[which].at[pl.ds(start, size), part], kept.at[pl.ds(at, size), part], rsem.at[k, m])
            at += size

    def copies(step, slot):
        at = 0
        cols = pl.ds(pl.multiple_of(step * tile, tile), tile)
        for k, (which, start, size) in enumerate(spieces):
            yield pltpu.make_async_copy(stream[which].at[pl.ds(start, size), cols], buf.at[slot, pl.ds(at, size)], ssem.at[slot, k])
            at += size

    slot = lax.rem(j, 2)

    @pl.when(j == 0)
    def _():
        for c in copies(0, 0):
            c.start()
        for m in range(3):
            for c in res_copies(m):
                c.start()

    @pl.when(j + 1 < steps)
    def _():
        for c in copies(j + 1, 1 - slot):
            c.start()

    for c in copies(j, slot):
        c.wait()
    for total, parts in zip(totals, addends):
        total[...] = sum(p[...].astype(F32) for p in parts).astype(total.dtype)

    if not resident_left:

        @pl.when(j == 0)
        def _():
            left[...] = buf[slot].T
            for m in range(3):
                for c in res_copies(m):
                    c.wait()
                part = slice(m * chunk, (m + 1) * chunk)
                out[:, part] = jnp.dot(left[...], kept[:, part], preferred_element_type=F32).astype(BF)

        @pl.when(j > 0)
        def _():
            out[...] = tn(buf[slot], kept[...]).astype(BF)

        return

    @pl.when(j == 0)
    def _():
        for m in range(3):
            for c in res_copies(m):
                c.wait()
            part = slice(m * chunk, (m + 1) * chunk)
            left[part] = kept[:, part].T
            out[part] = jnp.dot(left[part], buf[slot], preferred_element_type=F32).astype(BF)

    @pl.when(j > 0)
    def _():
        out[...] = jnp.dot(left[...], buf[slot], preferred_element_type=F32).astype(BF)


def weight_call(left, right, lpieces, rpieces, resident_left, sums=(), tile=512):
    (res, kept_pieces), (stream, moved_pieces) = ((left, lpieces), (right, rpieces)) if resident_left else ((right, rpieces), (left, lpieces))
    rows, kept, wide = sum(p[2] for p in kept_pieces), res[0].shape[1], stream[0].shape[1]
    if resident_left:
        out_shape, out_spec = (kept, wide), pl.BlockSpec((kept, tile), lambda j: (0, j))
    else:
        out_shape, out_spec = (wide, kept), pl.BlockSpec((tile, kept), lambda j: (j, 0))
    scratch = [
        pltpu.VMEM((rows, kept), BF),
        pltpu.VMEM((2, rows, tile), BF),
        pltpu.SemaphoreType.DMA((len(kept_pieces), 3)),
        pltpu.SemaphoreType.DMA((2, len(moved_pieces))),
        pltpu.VMEM((kept if resident_left else tile, rows), BF),
    ]
    return pl.pallas_call(
        functools.partial(weight_kernel, resident_left, len(res), len(stream), tile, tuple(kept_pieces), tuple(moved_pieces), tuple(len(s[0]) for s in sums)),
        out_shape=[jax.ShapeDtypeStruct(out_shape, BF)] + [jax.ShapeDtypeStruct((size, wide), t) for _, size, t in sums],
        grid=(wide // tile,),
        in_specs=[pl.BlockSpec(memory_space=pl.ANY)] * (len(res) + len(stream))
        + [pl.BlockSpec((size, tile), functools.partial(lambda b, j: (b, j), b)) for parts, size, _ in sums for _, b in parts],
        out_specs=[out_spec] + [pl.BlockSpec((size, tile), lambda j: (0, j)) for _, size, _ in sums],
        scratch_shapes=scratch,
        compiler_params=pltpu.CompilerParams(vmem_limit_bytes=LIMIT),
        cost_estimate=pl.CostEstimate(flops=2 * rows * kept * wide, bytes_accessed=2 * (rows * kept + rows * wide + kept * wide), transcendentals=0),
        name="weight",
    )(*res, *stream, *[a for parts, _, _ in sums for a, _ in parts])


X, Y, CORE = 4, 2, 1


def solution(mesh):
    spec = jax.sharding.PartitionSpec
    rows, cols = spec(("dp", "tp"), None), spec("dp", "tp")

    def flip(a, bit):
        return lax.ppermute(a, "tp", [(k, k ^ bit) for k in range(8)])

    def step(x, dy, gate, up, w_gate, w_up, w_down):
        n = x.shape[0]
        half = n // 2
        tie = lax.optimization_barrier
        hidden, d_gate, d_up, same, swapped, dys, xo, xa, xb, ya, yb = rows_call(dy, x, gate, up, w_down, w_gate, w_up)

        fwd = [flip(ya, X), flip(xb, Y)]
        near = [flip(p, CORE) for p in (xa, ya, xb, yb)]
        def term(block, *more, dtype=BF):
            return ((same, block), (swapped, block), *((m, 0) for m in more)), half, dtype

        whole = [(0, 0, 8 * n)]
        dw_down, *diag, near_x, near_y = weight_call([hidden], [dys], whole, whole, True, [term(6), term(7), term(2), term(5)])
        *fwd, near[0], near[1], near[2], near[3], diag[0], diag[1] = tie((*fwd, *near, *diag))
        r_lo, r_hi = flip(diag[0], X), flip(diag[1], Y)
        fwd += [flip(p, CORE) for p in fwd]
        *fwd, near_x, near_y = tie((*fwd, near_x, near_y))
        from_x, from_y = flip(near_x, X), flip(near_y, Y)
        xs = [x, xo, xa, ya, near[0], near[1], xb, yb, near[2], near[3], *fwd]
        pieces = [(k, 0, p.shape[0]) for k, p in enumerate(xs)]
        (dw_gate,) = weight_call(xs, [d_gate], pieces, whole, False)
        r_lo, r_hi, dw_gate = tie((r_lo, r_hi, dw_gate))

        def total(block, more):
            rows = slice(block * half, (block + 1) * half)
            return (same[rows] + swapped[rows].astype(F32) + more.astype(F32)).astype(BF)

        t_lo, t_hi, d_up = tie((total(3, r_lo), total(4, r_hi), d_up))
        last_lo, last_hi = flip(t_lo, Y), flip(t_hi, X)
        dw_up, base_lo, base_hi = weight_call(xs, [d_up], pieces, whole, False, [term(0, from_x, dtype=F32), term(1, from_y, dtype=F32)])
        dx = jnp.concatenate([base_lo + last_lo.astype(F32), base_hi + last_hi.astype(F32)])
        return dx.astype(BF), dw_gate, dw_up, dw_down

    return jax.shard_map(
        step,
        mesh=mesh,
        in_specs=(rows, rows, cols, cols, spec(None, "tp"), spec(None, "tp"), spec("tp", None)),
        out_specs=(rows, cols, cols, rows),
        check_vma=False,
    )
```

```python
import functools
import jax
import jax.numpy as jnp
from jax import lax
from jax.experimental import pallas as pl
from jax.experimental.pallas import tpu as pltpu

BF, F32 = jnp.bfloat16, jnp.float32
LIMIT = 62 * 1024 * 1024


def nt(a, b):
    return lax.dot_general(a, b, (((1,), (1,)), ((), ())), preferred_element_type=F32)


def tn(a, b):
    return lax.dot_general(a, b, (((0,), (0,)), ((), ())), preferred_element_type=F32)


def flipped(along_x, along_y, core):
    me = lax.axis_index("tp")
    return me + along_x * (4 - 8 * (me // 4)) + along_y * (2 - 4 * (me // 2 % 2)) + core * (1 - 2 * (me % 2))


def piece_row(g, k):
    core = k // 2
    own = 2 * flipped(0, 0, core) + k % 2
    near = 2 * (flipped(1, 0, core) if k % 2 == 0 else flipped(0, 1, core))
    diag = 2 * flipped(1, 1, core) + k % 2
    return jnp.where(g == 0, own, jnp.where(g == 3, diag, near + g - 1))


def order(g, i, n):
    i = jnp.clip(i, 0, n - 1)
    return i + (g % 2) * (n - 1 - 2 * i)


def rows_kernel(n1, n2, tf, td, half, events, dy, x, gate, up, wd, wg, wu, *refs):
    h_out, g_out, u_out, same, swapped, dyg, xo, xa, xb, ya, yb = refs[:11]
    rows, gates, ups, hid, dg, du, stage, send, recv, local, gsem, osem, acc, wd_buf, w_buf, wd_sem, w_sem = refs[11:]
    g, i = pl.program_id(0), pl.program_id(1)
    last = n1 + n2 - 1
    n = 2 * half
    to_x, to_y, partner = ({"tp": flipped(*f)} for f in ((1, 0, 0), (0, 1, 0), (0, 0, 1)))

    def remote(k, src, dst, device):
        return pltpu.make_async_remote_copy(
            src_ref=src, dst_ref=dst, send_sem=send.at[k], recv_sem=recv.at[k], device_id=device, device_id_type=pl.DeviceIdType.MESH
        )

    lo, hi, first_n, last_n = pl.ds(0, half), pl.ds(half, half), pl.ds(0, n), pl.ds(n, n)
    own_swap = remote(0, dy, rows.at[0, last_n], partner)
    lo_x, lo_y = remote(1, dy.at[lo], rows.at[1, lo], to_x), remote(2, dy.at[lo], rows.at[1, hi], to_y)
    hi_x, hi_y = remote(3, dy.at[hi], rows.at[2, lo], to_x), remote(4, dy.at[hi], rows.at[2, hi], to_y)
    swap1, on_x = remote(5, rows.at[1, first_n], rows.at[1, last_n], partner), remote(6, rows.at[1, hi], rows.at[3, lo], to_x)
    swap2, on_y = remote(7, rows.at[2, first_n], rows.at[2, last_n], partner), remote(8, rows.at[2, lo], rows.at[3, hi], to_y)
    swap3 = remote(9, rows.at[3, first_n], rows.at[3, last_n], partner)
    x_copies = [remote(10, x, xo, partner)]
    for src, at_x, at_y in ((x.at[lo], xa, ya), (x.at[hi], xb, yb)):
        k = 10 + len(x_copies)
        x_copies += [remote(k, src, at_x, to_x), remote(k + 1, src, at_y, to_y)]
    passes = []
    for group in range(4):
        final = 0 if group % 2 else (n2 - 1) * td
        early = pl.ds(td if group % 2 else 0, (n2 - 1) * td)
        out_rows = pl.ds(group * n, n)
        k = 15 + 2 * group
        passes.append([remote(k + j, stage.at[:, c], swapped.at[out_rows, c], partner) for j, c in enumerate((early, pl.ds(final, td)))])

    def kept(group):
        for k in range(4):
            at_rows = pl.ds(pl.multiple_of(piece_row(group, k) * half, half), half)
            for j, (ref, buf) in enumerate(((gate, gates), (up, ups))):
                yield pltpu.make_async_copy(ref.at[at_rows], buf.at[pl.ds(k * half, half)], gsem.at[j, k])

    def outs(group):
        for j, (buf, ref) in enumerate(((hid, h_out), (dg, g_out), (du, u_out))):
            yield pltpu.make_async_copy(buf, ref.at[pl.ds(pl.multiple_of(group * 2 * n, 2 * n), 2 * n)], osem.at[j])

    def tiles(sources, buf, sem, count, size, q):
        turn, at = q // (count - 1), q % (count - 1)
        start = (at + turn % 2 * (count - 1 - 2 * at)) * size
        for k, ref in enumerate(sources):
            yield pltpu.make_async_copy(ref.at[pl.ds(pl.multiple_of(start, size), size)], buf.at[q % 2, k], sem.at[q % 2, k])

    q1, q2 = g * (n1 - 1) + i, g * (n2 - 1) + i - n1
    first_tiles, second_tiles = functools.partial(tiles, [wd], wd_buf, wd_sem, n1, tf), functools.partial(tiles, [wg, wu], w_buf, w_sem, n2, td)

    take = pltpu.make_async_copy(dy, rows.at[0, first_n], local.at[4])
    keeps = [pltpu.make_async_copy(rows.at[k], dyg.at[pl.ds(2 * n * k, 2 * n)], local.at[k]) for k in range(4)]

    def at(group, step):
        return pl.when((g == group) & (i == step))

    @at(0, 0)
    def _():
        barrier = pltpu.get_barrier_semaphore()
        for device in (to_x, to_y, partner):
            pl.semaphore_signal(barrier, inc=1, device_id=device, device_id_type=pl.DeviceIdType.MESH)
        pl.semaphore_wait(barrier, 3)
        own_swap.start()
        lo_x.start()
        lo_y.start()
        take.start()
        for copies in (first_tiles(0), kept(0), second_tiles(0)):
            for copy in copies:
                copy.start()
        take.wait()
        own_swap.wait_recv()
        keeps[0].start()

    @at(0, events[0])
    def _():
        hi_x.start()
        hi_y.start()

    @at(0, events[1])
    def _():
        lo_x.wait_recv()
        lo_y.wait_recv()
        swap1.start()
        on_x.start()

    @at(1, 0)
    def _():
        swap1.wait_recv()
        keeps[1].start()

    @at(1, events[2])
    def _():
        hi_x.wait_recv()
        hi_y.wait_recv()
        swap2.start()
        on_y.start()
        for copy in x_copies:
            copy.start()

    @at(2, 0)
    def _():
        swap2.wait_recv()
        keeps[2].start()

    @at(2, events[3])
    def _():
        on_x.wait_recv()
        on_y.wait_recv()
        swap3.start()

    @at(3, 0)
    def _():
        swap3.wait_recv()
        keeps[3].start()

    for group in range(4):

        @at(group, last)
        def _(group=group):
            passes[group][0].start()

        @at(group + 1, 0)
        def _(group=group):
            passes[group][1].start()

        @at(group + 1, n1)
        def _(group=group):
            for copy in passes[group]:
                copy.wait_send()

    @pl.when(i == 0)
    def _():
        for copy in kept(g):
            copy.wait()

    @pl.when((i == 0) & (g > 0))
    def _():
        for copy in outs(g - 1):
            copy.wait()

    @pl.when(i == n1 + 1)
    def _():
        for copy in outs(g):
            copy.start()

    @pl.when((i == n1 + 1) & (g < 3))
    def _():
        for copy in kept(g + 1):
            copy.start()

    def activate(step):
        here = pl.ds(pl.multiple_of(order(g, step, n1) * tf, tf), tf)
        for k in range(4):
            part = slice(k * half, (k + 1) * half)
            d = acc[(step + 2) % 2, part]
            a, u = gates[part, here].astype(F32), ups[part, here].astype(F32)
            s = jax.nn.sigmoid(a)
            act = a * s
            hid[part, here] = (act * u).astype(BF)
            dg[part, here] = (d * u * (s + act * (1 - s))).astype(BF)
            du[part, here] = (d * act).astype(BF)

    @pl.when((i < n1) & ((g == 0) | (i > 0)))
    def _():
        for copy in first_tiles(q1):
            copy.wait()

        @pl.when(q1 < 4 * (n1 - 1))
        def _():
            for copy in first_tiles(q1 + 1):
                copy.start()

    @pl.when((i >= n1) & ((g == 0) | (i > n1)))
    def _():
        for copy in second_tiles(q2):
            copy.wait()

        @pl.when(q2 < 4 * (n2 - 1))
        def _():
            for copy in second_tiles(q2 + 1):
                copy.start()

    @pl.when(i < n1)
    def _():
        acc[i % 2] = nt(rows[g], wd_buf[q1 % 2, 0])
        activate(i - 1)

    @pl.when(i == n1)
    def _():
        activate(n1 - 1)

    @pl.when(i >= n1)
    def _():
        dx = nt(dg[...], w_buf[q2 % 2, 0]) + nt(du[...], w_buf[q2 % 2, 1])
        same[...] = dx[:n]
        stage[:, pl.ds(pl.multiple_of(order(g, i - n1, n2) * td, td), td)] = dx[n:].astype(BF)

    @at(3, last)
    def _():
        for copy in x_copies[:3]:
            copy.wait_recv()
        passes[3][1].start()
        for copy in x_copies[3:]:
            copy.wait_recv()
        for copy in (own_swap, lo_x, lo_y, hi_x, hi_y, swap1, on_x, swap2, on_y, swap3, *x_copies):
            copy.wait_send()
        for copy in keeps:
            copy.wait()
        for copy in outs(3):
            copy.wait()
        for copy in passes[3]:
            copy.wait_send()
        for pair in passes:
            for copy in pair:
                copy.wait_recv()


def rows_call(dy, x, gate, up, w_down, w_gate, w_up, tf=512, td=1024, events=(3, 7, 5, 5)):
    n, d = dy.shape
    ff = w_down.shape[0]
    n1, n2, half = ff // tf, d // td, n // 2
    dx_block = pl.BlockSpec((n, td), lambda g, i: (g, order(g, i - n1, n2)))
    hbm = pl.BlockSpec(memory_space=pl.ANY)
    return pl.pallas_call(
        functools.partial(rows_kernel, n1, n2, tf, td, half, events),
        out_shape=[jax.ShapeDtypeStruct((8 * n, ff), BF)] * 3
        + [jax.ShapeDtypeStruct((4 * n, d), F32), jax.ShapeDtypeStruct((4 * n, d), BF), jax.ShapeDtypeStruct((8 * n, d), BF), jax.ShapeDtypeStruct((n, d), BF)]
        + [jax.ShapeDtypeStruct((half, d), BF)] * 4,
        grid=(4, n1 + n2),
        in_specs=[hbm] * 7,
        out_specs=[hbm] * 3 + [dx_block] + [hbm] * 7,
        scratch_shapes=[
            pltpu.VMEM((4, 2 * n, d), BF),
            *[pltpu.VMEM((2 * n, ff), BF)] * 5,
            pltpu.VMEM((n, d), BF),
            pltpu.SemaphoreType.DMA((23,)),
            pltpu.SemaphoreType.DMA((23,)),
            pltpu.SemaphoreType.DMA((5,)),
            pltpu.SemaphoreType.DMA((2, 4)),
            pltpu.SemaphoreType.DMA((3,)),
            pltpu.VMEM((2, 2 * n, tf), F32),
            pltpu.VMEM((2, 1, tf, d), BF),
            pltpu.VMEM((2, 2, td, ff), BF),
            pltpu.SemaphoreType.DMA((2, 1)),
            pltpu.SemaphoreType.DMA((2, 2)),
        ],
        compiler_params=pltpu.CompilerParams(vmem_limit_bytes=LIMIT, collective_id=0, has_side_effects=True),
        cost_estimate=pl.CostEstimate(flops=48 * n * d * ff, bytes_accessed=24 * d * ff + 48 * n * (d + ff), transcendentals=8 * n * ff),
        name="rows",
    )(dy, x, gate, up, w_down, w_gate, w_up)


def weight_kernel(resident_left, nr, ns, tile, rpieces, spieces, sums, *refs):
    refs = list(refs)
    res, stream = [refs.pop(0) for _ in range(nr)], [refs.pop(0) for _ in range(ns)]
    addends = [[refs.pop(0) for _ in range(k)] for k in sums]
    out, *totals = [refs.pop(0) for _ in range(1 + len(sums))]
    kept, buf, rsem, ssem, left = refs
    j, steps = pl.program_id(0), pl.num_programs(0)

    chunk = kept.shape[1] // 3

    def res_copies(m):
        at, part = 0, pl.ds(m * chunk, chunk)
        for k, (which, start, size) in enumerate(rpieces):
            yield pltpu.make_async_copy(res[which].at[pl.ds(start, size), part], kept.at[pl.ds(at, size), part], rsem.at[k, m])
            at += size

    def copies(step, slot):
        at = 0
        cols = pl.ds(pl.multiple_of(step * tile, tile), tile)
        for k, (which, start, size) in enumerate(spieces):
            yield pltpu.make_async_copy(stream[which].at[pl.ds(start, size), cols], buf.at[slot, pl.ds(at, size)], ssem.at[slot, k])
            at += size

    slot = lax.rem(j, 2)

    @pl.when(j == 0)
    def _():
        for c in copies(0, 0):
            c.start()
        for m in range(3):
            for c in res_copies(m):
                c.start()

    @pl.when(j + 1 < steps)
    def _():
        for c in copies(j + 1, 1 - slot):
            c.start()

    for c in copies(j, slot):
        c.wait()
    for total, parts in zip(totals, addends):
        total[...] = sum(p[...].astype(F32) for p in parts).astype(total.dtype)

    if not resident_left:

        @pl.when(j == 0)
        def _():
            left[...] = buf[slot].T
            for m in range(3):
                for c in res_copies(m):
                    c.wait()
                part = slice(m * chunk, (m + 1) * chunk)
                out[:, part] = jnp.dot(left[...], kept[:, part], preferred_element_type=F32).astype(BF)

        @pl.when(j > 0)
        def _():
            out[...] = tn(buf[slot], kept[...]).astype(BF)

        return

    @pl.when(j == 0)
    def _():
        for m in range(3):
            for c in res_copies(m):
                c.wait()
            part = slice(m * chunk, (m + 1) * chunk)
            left[part] = kept[:, part].T
            out[part] = jnp.dot(left[part], buf[slot], preferred_element_type=F32).astype(BF)

    @pl.when(j > 0)
    def _():
        out[...] = jnp.dot(left[...], buf[slot], preferred_element_type=F32).astype(BF)


def weight_call(left, right, lpieces, rpieces, resident_left, sums=(), tile=512):
    (res, kept_pieces), (stream, moved_pieces) = ((left, lpieces), (right, rpieces)) if resident_left else ((right, rpieces), (left, lpieces))
    rows, kept, wide = sum(p[2] for p in kept_pieces), res[0].shape[1], stream[0].shape[1]
    if resident_left:
        out_shape, out_spec = (kept, wide), pl.BlockSpec((kept, tile), lambda j: (0, j))
    else:
        out_shape, out_spec = (wide, kept), pl.BlockSpec((tile, kept), lambda j: (j, 0))
    scratch = [
        pltpu.VMEM((rows, kept), BF),
        pltpu.VMEM((2, rows, tile), BF),
        pltpu.SemaphoreType.DMA((len(kept_pieces), 3)),
        pltpu.SemaphoreType.DMA((2, len(moved_pieces))),
        pltpu.VMEM((kept if resident_left else tile, rows), BF),
    ]
    return pl.pallas_call(
        functools.partial(weight_kernel, resident_left, len(res), len(stream), tile, tuple(kept_pieces), tuple(moved_pieces), tuple(len(s[0]) for s in sums)),
        out_shape=[jax.ShapeDtypeStruct(out_shape, BF)] + [jax.ShapeDtypeStruct((size, wide), t) for _, size, t in sums],
        grid=(wide // tile,),
        in_specs=[pl.BlockSpec(memory_space=pl.ANY)] * (len(res) + len(stream))
        + [pl.BlockSpec((size, tile), functools.partial(lambda b, j: (b, j), b)) for parts, size, _ in sums for _, b in parts],
        out_specs=[out_spec] + [pl.BlockSpec((size, tile), lambda j: (0, j)) for _, size, _ in sums],
        scratch_shapes=scratch,
        compiler_params=pltpu.CompilerParams(vmem_limit_bytes=LIMIT),
        cost_estimate=pl.CostEstimate(flops=2 * rows * kept * wide, bytes_accessed=2 * (rows * kept + rows * wide + kept * wide), transcendentals=0),
        name="weight",
    )(*res, *stream, *[a for parts, _, _ in sums for a, _ in parts])


X, Y, CORE = 4, 2, 1


def solution(mesh):
    spec = jax.sharding.PartitionSpec
    rows, cols = spec(("dp", "tp"), None), spec("dp", "tp")

    def flip(a, bit):
        return lax.ppermute(a, "tp", [(k, k ^ bit) for k in range(8)])

    def step(x, dy, gate, up, w_gate, w_up, w_down):
        n = x.shape[0]
        half = n // 2
        tie = lax.optimization_barrier
        hidden, d_gate, d_up, same, swapped, dys, xo, xa, xb, ya, yb = rows_call(dy, x, gate, up, w_down, w_gate, w_up)

        fwd = [flip(ya, X), flip(xb, Y)]
        near = [flip(p, CORE) for p in (xa, ya, xb, yb)]
        def term(block):
            return ((same, block), (swapped, block)), half, BF

        whole = [(0, 0, 8 * n)]
        dw_down, *diag, near_x, near_y = weight_call([hidden], [dys], whole, whole, True, [term(6), term(7), term(2), term(5)])
        *fwd, near[0], near[1], near[2], near[3], diag[0], diag[1] = tie((*fwd, *near, *diag))
        r_lo, r_hi = flip(diag[0], X), flip(diag[1], Y)
        fwd += [flip(p, CORE) for p in fwd]
        *fwd, near_x, near_y = tie((*fwd, near_x, near_y))
        from_x, from_y = flip(near_x, X), flip(near_y, Y)
        xs = [x, xo, xa, ya, near[0], near[1], xb, yb, near[2], near[3], *fwd]
        pieces = [(k, 0, p.shape[0]) for k, p in enumerate(xs)]
        (dw_gate,) = weight_call(xs, [d_gate], pieces, whole, False)
        r_lo, r_hi, dw_gate = tie((r_lo, r_hi, dw_gate))

        def total(block, more):
            rows = slice(block * half, (block + 1) * half)
            return (same[rows] + swapped[rows].astype(F32) + more.astype(F32)).astype(BF)

        t_lo, t_hi, d_up = tie((total(3, r_lo), total(4, r_hi), d_up))
        last_lo, last_hi = flip(t_lo, Y), flip(t_hi, X)
        dw_up, dx = weight_call(xs, [d_up], pieces, whole, False, [(((same, 0), (swapped, 0)), n, F32)])
        for parts in ((from_x, from_y), (last_lo, last_hi)):
            dx += jnp.concatenate(parts).astype(F32)
        return dx.astype(BF), dw_gate, dw_up, dw_down

    return jax.shard_map(
        step,
        mesh=mesh,
        in_specs=(rows, rows, cols, cols, spec(None, "tp"), spec(None, "tp"), spec("tp", None)),
        out_specs=(rows, cols, cols, rows),
        check_vma=False,
    )
```

```python
import functools
import jax
import jax.numpy as jnp
from jax import lax
from jax.experimental import pallas as pl
from jax.experimental.pallas import tpu as pltpu

BF, F32 = jnp.bfloat16, jnp.float32
LIMIT = 62 * 1024 * 1024


def nt(a, b):
    return lax.dot_general(a, b, (((1,), (1,)), ((), ())), preferred_element_type=F32)


def tn(a, b):
    return lax.dot_general(a, b, (((0,), (0,)), ((), ())), preferred_element_type=F32)


def flipped(along_x, along_y, core):
    me = lax.axis_index("tp")
    return me + along_x * (4 - 8 * (me // 4)) + along_y * (2 - 4 * (me // 2 % 2)) + core * (1 - 2 * (me % 2))


def piece_row(g, k):
    core = k // 2
    own = 2 * flipped(0, 0, core) + k % 2
    near = 2 * (flipped(1, 0, core) if k % 2 == 0 else flipped(0, 1, core))
    diag = 2 * flipped(1, 1, core) + k % 2
    return jnp.where(g == 0, own, jnp.where(g == 3, diag, near + g - 1))


def order(g, i, n):
    i = jnp.clip(i, 0, n - 1)
    return i + (g % 2) * (n - 1 - 2 * i)


def rows_kernel(n1, n2, tf, td, half, cut, events, dy, x, gate, up, wd, wg, wu, *refs):
    h_out, g_out, u_out, same, swapped, dyg, xo, xa, xb, ya, yb = refs[:11]
    rows, gates, ups, hid, dg, du, stage, send, recv, local, gsem, osem, acc, wd_buf, w_buf, wd_sem, w_sem = refs[11:]
    g, i = pl.program_id(0), pl.program_id(1)
    last = n1 + n2 - 1
    n = 2 * half
    to_x, to_y, partner = ({"tp": flipped(*f)} for f in ((1, 0, 0), (0, 1, 0), (0, 0, 1)))

    def remote(k, src, dst, device):
        return pltpu.make_async_remote_copy(
            src_ref=src, dst_ref=dst, send_sem=send.at[k], recv_sem=recv.at[k], device_id=device, device_id_type=pl.DeviceIdType.MESH
        )

    lo, hi, first_n, last_n = pl.ds(0, half), pl.ds(half, half), pl.ds(0, n), pl.ds(n, n)
    own_swap = remote(0, dy, rows.at[0, last_n], partner)
    lo_x, lo_y = remote(1, dy.at[lo], rows.at[1, lo], to_x), remote(2, dy.at[lo], rows.at[1, hi], to_y)
    hi_x, hi_y = remote(3, dy.at[hi], rows.at[2, lo], to_x), remote(4, dy.at[hi], rows.at[2, hi], to_y)
    swap1, on_x = remote(5, rows.at[1, first_n], rows.at[1, last_n], partner), remote(6, rows.at[1, hi], rows.at[3, lo], to_x)
    swap2, on_y = remote(7, rows.at[2, first_n], rows.at[2, last_n], partner), remote(8, rows.at[2, lo], rows.at[3, hi], to_y)
    swap3 = remote(9, rows.at[3, first_n], rows.at[3, last_n], partner)
    x_copies = [remote(10, x, xo, partner), remote(11, x.at[hi], xb, to_x), remote(12, x.at[lo], ya, to_y)]
    x_copies += [remote(13, x.at[pl.ds(0, cut)], xa, to_x), remote(14, x.at[pl.ds(half, cut)], yb, to_y)]
    passes = []
    for group in range(4):
        final = 0 if group % 2 else (n2 - 1) * td
        early = pl.ds(td if group % 2 else 0, (n2 - 1) * td)
        out_rows = pl.ds(group * n, n)
        k = 15 + 2 * group
        passes.append([remote(k + j, stage.at[:, c], swapped.at[out_rows, c], partner) for j, c in enumerate((early, pl.ds(final, td)))])

    def kept(group):
        for k in range(4):
            at_rows = pl.ds(pl.multiple_of(piece_row(group, k) * half, half), half)
            for j, (ref, buf) in enumerate(((gate, gates), (up, ups))):
                yield pltpu.make_async_copy(ref.at[at_rows], buf.at[pl.ds(k * half, half)], gsem.at[j, k])

    def outs(group):
        for j, (buf, ref) in enumerate(((hid, h_out), (dg, g_out), (du, u_out))):
            yield pltpu.make_async_copy(buf, ref.at[pl.ds(pl.multiple_of(group * 2 * n, 2 * n), 2 * n)], osem.at[j])

    def tiles(sources, buf, sem, count, size, q):
        turn, at = q // (count - 1), q % (count - 1)
        start = (at + turn % 2 * (count - 1 - 2 * at)) * size
        for k, ref in enumerate(sources):
            yield pltpu.make_async_copy(ref.at[pl.ds(pl.multiple_of(start, size), size)], buf.at[q % 2, k], sem.at[q % 2, k])

    q1, q2 = g * (n1 - 1) + i, g * (n2 - 1) + i - n1
    first_tiles, second_tiles = functools.partial(tiles, [wd], wd_buf, wd_sem, n1, tf), functools.partial(tiles, [wg, wu], w_buf, w_sem, n2, td)

    take = pltpu.make_async_copy(dy, rows.at[0, first_n], local.at[4])
    keeps = [pltpu.make_async_copy(rows.at[k], dyg.at[pl.ds(2 * n * k, 2 * n)], local.at[k]) for k in range(4)]

    def at(group, step):
        return pl.when((g == group) & (i == step))

    @at(0, 0)
    def _():
        barrier = pltpu.get_barrier_semaphore()
        for device in (to_x, to_y, partner):
            pl.semaphore_signal(barrier, inc=1, device_id=device, device_id_type=pl.DeviceIdType.MESH)
        pl.semaphore_wait(barrier, 3)
        own_swap.start()
        lo_x.start()
        lo_y.start()
        take.start()
        for copies in (first_tiles(0), kept(0), second_tiles(0)):
            for copy in copies:
                copy.start()
        take.wait()
        own_swap.wait_recv()
        keeps[0].start()

    @at(0, events[0])
    def _():
        hi_x.start()
        hi_y.start()

    @at(0, events[1])
    def _():
        lo_x.wait_recv()
        lo_y.wait_recv()
        swap1.start()
        on_x.start()

    @at(1, 0)
    def _():
        swap1.wait_recv()
        keeps[1].start()

    @at(1, events[2])
    def _():
        hi_x.wait_recv()
        hi_y.wait_recv()
        swap2.start()
        on_y.start()
        for copy in x_copies:
            copy.start()

    @at(2, 0)
    def _():
        swap2.wait_recv()
        keeps[2].start()

    @at(2, events[3])
    def _():
        on_x.wait_recv()
        on_y.wait_recv()
        swap3.start()

    @at(3, 0)
    def _():
        swap3.wait_recv()
        keeps[3].start()

    for group in range(4):

        @at(group, last)
        def _(group=group):
            passes[group][0].start()

        @at(group + 1, 0)
        def _(group=group):
            passes[group][1].start()

        @at(group + 1, n1)
        def _(group=group):
            for copy in passes[group]:
                copy.wait_send()

    @pl.when(i == 0)
    def _():
        for copy in kept(g):
            copy.wait()

    @pl.when((i == 0) & (g > 0))
    def _():
        for copy in outs(g - 1):
            copy.wait()

    @pl.when(i == n1 + 1)
    def _():
        for copy in outs(g):
            copy.start()

    @pl.when((i == n1 + 1) & (g < 3))
    def _():
        for copy in kept(g + 1):
            copy.start()

    def activate(step):
        here = pl.ds(pl.multiple_of(order(g, step, n1) * tf, tf), tf)
        for k in range(4):
            part = slice(k * half, (k + 1) * half)
            d = acc[(step + 2) % 2, part]
            a, u = gates[part, here].astype(F32), ups[part, here].astype(F32)
            s = jax.nn.sigmoid(a)
            act = a * s
            hid[part, here] = (act * u).astype(BF)
            dg[part, here] = (d * u * (s + act * (1 - s))).astype(BF)
            du[part, here] = (d * act).astype(BF)

    @pl.when((i < n1) & ((g == 0) | (i > 0)))
    def _():
        for copy in first_tiles(q1):
            copy.wait()

        @pl.when(q1 < 4 * (n1 - 1))
        def _():
            for copy in first_tiles(q1 + 1):
                copy.start()

    @pl.when((i >= n1) & ((g == 0) | (i > n1)))
    def _():
        for copy in second_tiles(q2):
            copy.wait()

        @pl.when(q2 < 4 * (n2 - 1))
        def _():
            for copy in second_tiles(q2 + 1):
                copy.start()

    @pl.when(i < n1)
    def _():
        acc[i % 2] = nt(rows[g], wd_buf[q1 % 2, 0])
        activate(i - 1)

    @pl.when(i == n1)
    def _():
        activate(n1 - 1)

    @pl.when(i >= n1)
    def _():
        dx = nt(dg[...], w_buf[q2 % 2, 0]) + nt(du[...], w_buf[q2 % 2, 1])
        same[...] = dx[:n]
        stage[:, pl.ds(pl.multiple_of(order(g, i - n1, n2) * td, td), td)] = dx[n:].astype(BF)

    @at(3, last)
    def _():
        for copy in x_copies[:3]:
            copy.wait_recv()
        passes[3][1].start()
        for copy in x_copies[3:]:
            copy.wait_recv()
        for copy in (own_swap, lo_x, lo_y, hi_x, hi_y, swap1, on_x, swap2, on_y, swap3, *x_copies):
            copy.wait_send()
        for copy in keeps:
            copy.wait()
        for copy in outs(3):
            copy.wait()
        for copy in passes[3]:
            copy.wait_send()
        for pair in passes:
            for copy in pair:
                copy.wait_recv()


def rows_call(dy, x, gate, up, w_down, w_gate, w_up, cut, tf=512, td=1024, events=(3, 7, 5, 5)):
    n, d = dy.shape
    ff = w_down.shape[0]
    n1, n2, half = ff // tf, d // td, n // 2
    dx_block = pl.BlockSpec((n, td), lambda g, i: (g, order(g, i - n1, n2)))
    hbm = pl.BlockSpec(memory_space=pl.ANY)
    return pl.pallas_call(
        functools.partial(rows_kernel, n1, n2, tf, td, half, cut, events),
        out_shape=[jax.ShapeDtypeStruct((8 * n, ff), BF)] * 3
        + [jax.ShapeDtypeStruct((4 * n, d), F32), jax.ShapeDtypeStruct((4 * n, d), BF), jax.ShapeDtypeStruct((8 * n, d), BF), jax.ShapeDtypeStruct((n, d), BF)]
        + [jax.ShapeDtypeStruct((rows, d), BF) for rows in (cut, half, half, cut)],
        grid=(4, n1 + n2),
        in_specs=[hbm] * 7,
        out_specs=[hbm] * 3 + [dx_block] + [hbm] * 7,
        scratch_shapes=[
            pltpu.VMEM((4, 2 * n, d), BF),
            *[pltpu.VMEM((2 * n, ff), BF)] * 5,
            pltpu.VMEM((n, d), BF),
            pltpu.SemaphoreType.DMA((23,)),
            pltpu.SemaphoreType.DMA((23,)),
            pltpu.SemaphoreType.DMA((5,)),
            pltpu.SemaphoreType.DMA((2, 4)),
            pltpu.SemaphoreType.DMA((3,)),
            pltpu.VMEM((2, 2 * n, tf), F32),
            pltpu.VMEM((2, 1, tf, d), BF),
            pltpu.VMEM((2, 2, td, ff), BF),
            pltpu.SemaphoreType.DMA((2, 1)),
            pltpu.SemaphoreType.DMA((2, 2)),
        ],
        compiler_params=pltpu.CompilerParams(vmem_limit_bytes=LIMIT, collective_id=0, has_side_effects=True),
        cost_estimate=pl.CostEstimate(flops=48 * n * d * ff, bytes_accessed=24 * d * ff + 48 * n * (d + ff), transcendentals=8 * n * ff),
        name="rows",
    )(dy, x, gate, up, w_down, w_gate, w_up)


def weight_kernel(resident_left, nr, ns, tile, rpieces, spieces, sums, *refs):
    refs = list(refs)
    res, stream = [refs.pop(0) for _ in range(nr)], [refs.pop(0) for _ in range(ns)]
    addends = [[refs.pop(0) for _ in range(k)] for k in sums]
    out, *totals = [refs.pop(0) for _ in range(1 + len(sums))]
    kept, buf, rsem, ssem, left = refs
    j, steps = pl.program_id(0), pl.num_programs(0)

    chunk = kept.shape[1] // 3

    def res_copies(m):
        at, part = 0, pl.ds(m * chunk, chunk)
        for k, (which, start, size) in enumerate(rpieces):
            yield pltpu.make_async_copy(res[which].at[pl.ds(start, size), part], kept.at[pl.ds(at, size), part], rsem.at[k, m])
            at += size

    def copies(step, slot):
        at = 0
        cols = pl.ds(pl.multiple_of(step * tile, tile), tile)
        for k, (which, start, size) in enumerate(spieces):
            yield pltpu.make_async_copy(stream[which].at[pl.ds(start, size), cols], buf.at[slot, pl.ds(at, size)], ssem.at[slot, k])
            at += size

    slot = lax.rem(j, 2)

    @pl.when(j == 0)
    def _():
        for c in copies(0, 0):
            c.start()
        for m in range(3):
            for c in res_copies(m):
                c.start()

    @pl.when(j + 1 < steps)
    def _():
        for c in copies(j + 1, 1 - slot):
            c.start()

    for c in copies(j, slot):
        c.wait()
    for total, parts in zip(totals, addends):
        total[...] = sum(p[...].astype(F32) for p in parts).astype(total.dtype)

    if not resident_left:

        @pl.when(j == 0)
        def _():
            left[...] = buf[slot].T
            for m in range(3):
                for c in res_copies(m):
                    c.wait()
                part = slice(m * chunk, (m + 1) * chunk)
                out[:, part] = jnp.dot(left[...], kept[:, part], preferred_element_type=F32).astype(BF)

        @pl.when(j > 0)
        def _():
            out[...] = tn(buf[slot], kept[...]).astype(BF)

        return

    @pl.when(j == 0)
    def _():
        for m in range(3):
            for c in res_copies(m):
                c.wait()
            part = slice(m * chunk, (m + 1) * chunk)
            left[part] = kept[:, part].T
            out[part] = jnp.dot(left[part], buf[slot], preferred_element_type=F32).astype(BF)

    @pl.when(j > 0)
    def _():
        out[...] = jnp.dot(left[...], buf[slot], preferred_element_type=F32).astype(BF)


def weight_call(left, right, lpieces, rpieces, resident_left, sums=(), tile=512):
    (res, kept_pieces), (stream, moved_pieces) = ((left, lpieces), (right, rpieces)) if resident_left else ((right, rpieces), (left, lpieces))
    rows, kept, wide = sum(p[2] for p in kept_pieces), res[0].shape[1], stream[0].shape[1]
    if resident_left:
        out_shape, out_spec = (kept, wide), pl.BlockSpec((kept, tile), lambda j: (0, j))
    else:
        out_shape, out_spec = (wide, kept), pl.BlockSpec((tile, kept), lambda j: (j, 0))
    scratch = [
        pltpu.VMEM((rows, kept), BF),
        pltpu.VMEM((2, rows, tile), BF),
        pltpu.SemaphoreType.DMA((len(kept_pieces), 3)),
        pltpu.SemaphoreType.DMA((2, len(moved_pieces))),
        pltpu.VMEM((kept if resident_left else tile, rows), BF),
    ]
    return pl.pallas_call(
        functools.partial(weight_kernel, resident_left, len(res), len(stream), tile, tuple(kept_pieces), tuple(moved_pieces), tuple(len(s[0]) for s in sums)),
        out_shape=[jax.ShapeDtypeStruct(out_shape, BF)] + [jax.ShapeDtypeStruct((size, wide), t) for _, size, t in sums],
        grid=(wide // tile,),
        in_specs=[pl.BlockSpec(memory_space=pl.ANY)] * (len(res) + len(stream))
        + [pl.BlockSpec((size, tile), functools.partial(lambda b, j: (b, j), b)) for parts, size, _ in sums for _, b in parts],
        out_specs=[out_spec] + [pl.BlockSpec((size, tile), lambda j: (0, j)) for _, size, _ in sums],
        scratch_shapes=scratch,
        compiler_params=pltpu.CompilerParams(vmem_limit_bytes=LIMIT),
        cost_estimate=pl.CostEstimate(flops=2 * rows * kept * wide, bytes_accessed=2 * (rows * kept + rows * wide + kept * wide), transcendentals=0),
        name="weight",
    )(*res, *stream, *[a for parts, _, _ in sums for a, _ in parts])


X, Y, CORE = 4, 2, 1


def solution(mesh):
    spec = jax.sharding.PartitionSpec
    rows, cols = spec(("dp", "tp"), None), spec("dp", "tp")

    def flip(a, bit):
        return lax.ppermute(a, "tp", [(k, k ^ bit) for k in range(8)])

    def step(x, dy, gate, up, w_gate, w_up, w_down):
        n = x.shape[0]
        half = n // 2
        tie = lax.optimization_barrier
        cut = 64
        hidden, d_gate, d_up, same, swapped, dys, xo, xa, xb, ya, yb = rows_call(dy, x, gate, up, w_down, w_gate, w_up, cut)

        fwd = [flip(ya, X), flip(xb, Y)]
        near = [flip(p, CORE) for p in (xa, ya, xb, yb)]
        rest_lo, rest_hi, dys = tie((x[cut:half], x[half + cut :], dys))
        late = fwd + [flip(rest_lo, X), flip(rest_hi, Y)]

        def term(block):
            return ((same, block), (swapped, block)), half, BF

        whole = [(0, 0, 8 * n)]
        dw_down, *diag, near_x, near_y = weight_call([hidden], [dys], whole, whole, True, [term(6), term(7), term(2), term(5)])
        (late, near, diag) = tie((late, near, diag))
        r_lo, r_hi = flip(diag[0], X), flip(diag[1], Y)
        late += [flip(p, CORE) for p in late]
        late, near_x, near_y = tie((late, near_x, near_y))
        from_x, from_y = flip(near_x, X), flip(near_y, Y)
        xs = [x, xo, xa, late[2], ya, near[0], late[6], near[1]]
        xs += [xb, yb, late[3], near[2], near[3], late[7], late[0], late[1], late[4], late[5]]
        pieces = [(k, 0, p.shape[0]) for k, p in enumerate(xs)]
        (dw_gate,) = weight_call(xs, [d_gate], pieces, whole, False)
        r_lo, r_hi, dw_gate = tie((r_lo, r_hi, dw_gate))

        def total(block, more):
            rows = slice(block * half, (block + 1) * half)
            return (same[rows] + swapped[rows].astype(F32) + more.astype(F32)).astype(BF)

        t_lo, t_hi, d_up = tie((total(3, r_lo), total(4, r_hi), d_up))
        last_lo, last_hi = flip(t_lo, Y), flip(t_hi, X)
        dw_up, dx = weight_call(xs, [d_up], pieces, whole, False, [(((same, 0), (swapped, 0)), n, F32)])
        for parts in ((from_x, from_y), (last_lo, last_hi)):
            dx += jnp.concatenate(parts).astype(F32)
        return dx.astype(BF), dw_gate, dw_up, dw_down

    return jax.shard_map(
        step,
        mesh=mesh,
        in_specs=(rows, rows, cols, cols, spec(None, "tp"), spec(None, "tp"), spec("tp", None)),
        out_specs=(rows, cols, cols, rows),
        check_vma=False,
    )
```
